256 devices in a mesh: row: 32 (over z_hi, y, x), col: 8 (over z_lo, core).
Axes of the slice: x: 4, y: 4, z: 8 (z_hi: 2, z_lo: 4; z = z_hi * 4 + z_lo), core: 2. Of those that a mesh axis runs over, the one named last changes fastest.
Arguments:
- deltas: bfloat16 [256, 2, 3584, 512], P(('row', 'col')), may hold values from -192 to 192
- ages: int32 [32, 8], P('row', 'col'), may hold values from 0 to 7
- table: float32 [8], replicated, may hold values from 0.05 to 1
- params: float32 [2, 3584, 512], P(None, ('row', 'col')), may hold values from -6 to 6
- momentum: float32 [2, 3584, 512], P(None, ('row', 'col')), may hold values from -6 to 6
Outputs:
- new_params: float32 [2, 3584, 512], P(None, ('row', 'col'))
- new_momentum: float32 [2, 3584, 512], P(None, ('row', 'col'))
The draws below stay inside these ranges and needn't reach their ends.
All inputs are finite; a program needn't handle non-finite values.
Results may differ from the reference program's by a relative error of at most 0.0003.
Values sent between devices are 32-bit elements; how exact they have to be, the bound alone decides.
A program may use at most 128 MiB of HBM per device.

```python
import math
import jax
import jax.numpy as jnp
from jax import lax

D = 3584
KV = 512
PROJ = 2
AGES = 8
GROUPS = 256
N_ROW = 32
N_COL = 8


def place_ends(entries, key, least, high):
    index_at = [jax.random.randint(jax.random.fold_in(key, axis), (), 0, length) for axis, length in enumerate(entries.shape)]
    longest = entries.shape.index(max(entries.shape))
    neighbour = index_at[:longest] + [(index_at[longest] + 1) % entries.shape[longest]] + index_at[longest + 1:]
    return entries.at[tuple(index_at)].set(least).at[tuple(neighbour)].set(high)


def spiked(values, key, source, target, shards_of, factor):
    owner, partner = [(jnp.arange(values.shape[position]) // (values.shape[position] // shards_of)).reshape([-1 if axis == position else 1 for axis in range(values.ndim)]) for position in (source, target)]
    chosen = jax.random.permutation(key, shards_of)[partner]
    strong = (owner == chosen) | (owner == (partner + shards_of // 2) % shards_of)
    return jnp.where(strong, factor * values, values)


def block_levels(key, extent, cuts, least, largest):
    def one(axis_at, parts):
        steps = jax.random.uniform(jax.random.fold_in(jax.random.fold_in(key, 6), axis_at), (parts,), jnp.float32, least / len(cuts), largest / len(cuts))
        return jnp.repeat(jnp.exp(steps), extent[axis_at] // parts).reshape((-1,) + (1,) * (len(extent) - axis_at - 1))

    loudness = one(*cuts[0])
    for cut in cuts[1:]:
        loudness = loudness * one(*cut)
    return loudness


def centred(rng, extent, deviation, bound, split=(), kind=jnp.bfloat16):
    entries = deviation * jax.random.normal(rng, extent, jnp.float32)
    if split:
        entries = entries * block_levels(rng, extent, split, -0.22, 0.18)
    return jnp.clip(entries, -bound, bound).astype(kind)


def heavy_noise(own_key, dims, spread, most, cuts, heavy, held_as=jnp.bfloat16):
    drawn = spread * jax.random.normal(own_key, dims, jnp.float32)
    if cuts:
        drawn = drawn * block_levels(own_key, dims, cuts, -0.22, 0.18)
    return jnp.clip(spiked(drawn, jax.random.fold_in(own_key, 3), *heavy), -most, most).astype(held_as)


def setup_inputs(seed: int = 0) -> dict:
    splits = jax.random.split(jax.random.key(seed), 6)
    deltas = heavy_noise(splits[0], (GROUPS, PROJ, D, KV), 8.0, 192.0, ((0, 256),), (0, 2, 256, 6.0))
    ages = place_ends(jax.random.randint(splits[1], (N_ROW, N_COL), 0, AGES), jax.random.fold_in(splits[1], 1), 0, AGES - 1).astype(jnp.int32)
    table = jnp.clip(jnp.exp(jax.random.uniform(splits[2], (AGES,), jnp.float32, math.log(0.05), math.log(1.0))), 0.05, 1.0)
    params = centred(splits[3], (PROJ, D, KV), 1.0, 6.0, ((1, 256),), jnp.float32)
    momentum = centred(splits[4], (PROJ, D, KV), 1.0, 6.0, ((1, 256),), jnp.float32)
    return dict(deltas=deltas, ages=ages, table=table, params=params, momentum=momentum)


momentum_decay = 0.9
outer_rate = 0.7


def reference(deltas, ages, table, params, momentum):
    level = jnp.arange(AGES, dtype=jnp.int32)
    flat_ages = ages.reshape(-1).astype(jnp.int32)
    weights = jnp.sum(jnp.where(flat_ages[:, None] == level[None, :], table[None, :], jnp.zeros((), table.dtype)), axis=1)
    total = jnp.sum(weights)

    def accumulate(carry, item):
        weight, delta = item
        return carry + weight * delta.astype(carry.dtype), None

    start = jnp.zeros(deltas.shape[1:], table.dtype)
    summed, _ = lax.scan(accumulate, start, (weights, deltas))
    merged = summed / total
    new_momentum = momentum_decay * momentum + merged
    new_params = params - outer_rate * (merged + momentum_decay * new_momentum)
    return new_params, new_momentum
```

```python
import functools

import jax
import jax.numpy as jnp
from jax import lax
from jax.experimental import pallas as pl
from jax.experimental.pallas import tpu as pltpu
from jax.sharding import Mesh
from jax.sharding import PartitionSpec as P

ROW = ("z_hi", "y", "x")
COL = ("z_lo", "core")
ROW_COL = ROW + COL
MESH = pl.DeviceIdType.MESH
F32 = jnp.float32

momentum_decay = 0.9
outer_rate = 0.7

BLOCK = 112
WIN = 32
N_SEM = 160
A, B, C, D = range(4)


def kernel(delta, ages, table, out, theirs, ours, give, got, mine, t1, t2, tc, u2, zr,
           g1, g1c, g2, g2c, fin, wt, wx, send_sems, recv_sems, load_sems):
    zh, y, x, zl, core = [lax.axis_index(name) for name in ROW_COL]
    z = zh * 4 + zl
    barrier = pltpu.get_barrier_semaphore()

    load_theirs = pltpu.make_async_copy(delta.at[0, 1 - core], theirs, load_sems.at[0])
    load_ours = pltpu.make_async_copy(delta.at[0, core], ours, load_sems.at[1])
    load_theirs.start()
    load_ours.start()

    def at_z(there):
        there = lax.rem(there + 16, 8)
        return (there // 4, y, x, lax.rem(there, 4), core)

    def at_axis(is_x, step):
        return (zh, lax.rem(y + (1 - is_x) * step + 4, 4), lax.rem(x + is_x * step + 4, 4), zl, core)

    partner = (zh, y, x, zl, 1 - core)
    peers = [partner]
    peers += [at_axis(1, s) for s in (1, 2, 3)] + [at_axis(0, s) for s in (1, 2, 3)]
    peers += [at_z(z + s) for s in range(1, 8)]
    for peer in peers:
        pl.semaphore_signal(barrier, inc=1, device_id=peer, device_id_type=MESH)

    weight = table[ages[0, 0]]
    wt[0] = jnp.full((8, 128), weight, F32)

    sent = []

    def send(src, dst, device):
        i = len(sent)
        copy = pltpu.make_async_remote_copy(
            src_ref=src, dst_ref=dst, send_sem=send_sems.at[i], recv_sem=recv_sems.at[i],
            device_id=device, device_id_type=MESH)
        copy.start()
        sent.append(copy)
        return copy

    first = {A: 1, B: 0, C: 1 - core, D: 1 - core}
    first_of_partner = {A: 1, B: 0, C: core, D: core}

    def along(is_x):
        return is_x * x + (1 - is_x) * y

    def across(is_x):
        return is_x * y + (1 - is_x) * x

    def wrap4(value):
        return lax.rem(value + 4, 4)

    def block_of(unit, is_x, slot):
        if unit == C:
            half, d, j = slot // 16, lax.rem(slot, 16) // 4, lax.rem(slot, 4)
        else:
            d, half, j = slot // 8, lax.rem(slot, 8) // 4, lax.rem(slot, 4)
        return half * 16 + j * (4 * is_x + (1 - is_x)) + d * (is_x + 4 * (1 - is_x))

    def term(src, unit, is_x, slot):
        start = pl.multiple_of(block_of(unit, is_x, slot) * BLOCK, 16)
        return src[pl.ds(start, BLOCK), unit * 128:(unit + 1) * 128].astype(F32) * weight

    def chunk(unit, is_x, step):
        if unit == C:
            return lax.rem(zh + step, 2) * 16, 16
        return wrap4(along(is_x) + step) * 8, 8

    order = [(A, 2), (B, 2), (C, 1), (A, 1), (A, -1), (B, 1), (B, -1), (C, 0),
             (D, 2), (D, 1), (D, -1), (A, 0), (B, 0), (D, 0)]

    load_theirs.wait()
    swaps = {}
    for n, (unit, step) in enumerate(order):
        is_x = first_of_partner[unit]
        base, count = chunk(unit, is_x, step)

        @pl.loop(0, count)
        def _(k):
            give[unit, base + k] = term(theirs, unit, is_x, base + k)

        if n == 0:
            pl.semaphore_wait(barrier, len(peers))
        swaps[unit, step] = send(give.at[unit, pl.ds(base, count)], got.at[unit, pl.ds(base, count)], partner)
    swap_weight = send(wt.at[0], wt.at[1], partner)
    load_ours.wait()

    def settle(unit, step):
        is_x = first[unit]
        base, count = chunk(unit, is_x, step)
        swaps[unit, step].wait_recv()

        @pl.loop(0, count)
        def _(k):
            mine[unit, base + k] = got[unit, base + k] + term(ours, unit, is_x, base + k)

    class Tree:
        def __init__(self, piece, slots, is_x, me):
            self.piece, self.slots, self.is_x, self.me = piece, slots, is_x, me
            self.m0, self.m1, self.m2 = {}, {}, {}

        def far(self):
            for s in (1, -1):
                src = self.piece(s < 0, wrap4(self.me + 2))
                self.m0[s] = send(src, self.slots.at[0, int(s < 0)], at_axis(self.is_x, s))

        def near(self):
            for s in (1, -1):
                src = self.piece(s > 0, wrap4(self.me + s))
                self.m1[s] = send(src, self.slots.at[1, int(s < 0)], at_axis(self.is_x, s))

        def relay(self):
            for s in (1, -1):
                self.m0[s].wait_recv()
                held = self.slots.at[0, int(s < 0)]
                held[...] = held[...] + self.piece(s < 0, wrap4(self.me + s))[...]
                self.m2[s] = send(held, self.slots.at[2, int(s < 0)], at_axis(self.is_x, s))

        def finish(self, put):
            for s in (1, -1):
                self.m1[s].wait_recv()
                self.m2[s].wait_recv()
            for h in (0, 1):
                put(h, self.piece(h, self.me)[...] + self.slots[2, h] + self.slots[1, 1 - h])

    def first_tree(n, unit):
        is_x = first[unit]
        return Tree(lambda h, d: mine.at[unit, pl.ds(d * 8 + int(h) * 4, 4)], t1.at[n], is_x, along(is_x))

    def second_tree(n, unit):
        is_x = first[unit]
        return Tree(lambda h, d: g1.at[n, int(h), d], t2.at[n], 1 - is_x, across(is_x))

    trees1 = {unit: first_tree(n, unit) for n, unit in enumerate((A, B, D))}
    trees2 = {unit: second_tree(n, unit) for n, unit in enumerate((A, B, D))}
    place = {A: 0, B: 1, D: 2}

    def end_first(unit):
        def put(h, value):
            g1[place[unit], h] = value
        trees1[unit].finish(put)

    def end_second(unit):
        def put(h, value):
            g2[place[unit], h] = value
        trees2[unit].finish(put)

    dist = (4, 3, 3, 2, 2, 1, 1)

    def window(there):
        there = lax.rem(there + 16, 8)
        low = lax.rem(there, 4)
        return there // 4, pl.multiple_of((low // 2) * 56 + lax.rem(low, 2) * 24, 8)

    def c_piece(there, half):
        up, start = window(there)
        return mine.at[C, pl.ds(up * 16 + half * 8, 8), pl.ds(start, WIN)]

    def c_half(s, i):
        return int(s < 0) if i % 2 == 0 else int(s > 0)

    c_sent = {}

    def c_step(i):
        for s in (1, -1):
            n = int(s < 0)
            piece = c_piece(z + s * dist[i], c_half(s, i))
            if i >= 2:
                c_sent[s, i - 2].wait_recv()
                held = tc.at[n, i - 2]
                held[...] = held[...] + piece[...]
                piece = held
            c_sent[s, i] = send(piece, tc.at[n, i], at_z(z + s))

    def c_finish():
        for i in (5, 6):
            for s in (1, -1):
                c_sent[s, i].wait_recv()
        for half in (0, 1):
            g1c[half * 8:half * 8 + 8] = c_piece(z, half)[...] + tc[half, 6] + tc[1 - half, 5]

    c_x = first[C]
    tree_c = Tree(lambda h, d: g1c.at[pl.ds(d * 4 + int(h) * 2, 2)], u2, c_x, along(c_x))
    c_last = []

    def c_second_end():
        def put(h, value):
            g2c[h * 2:h * 2 + 2] = value
        tree_c.finish(put)
        for s in (2, 1, 3):
            c_last.append(send(g2c.at[wrap4(across(c_x) + s)], g2c.at[3 + s], at_axis(1 - c_x, s)))

    def c_end():
        for copy in c_last:
            copy.wait_recv()
        fin[core, C] = g2c[across(c_x)] + (g2c[4] + g2c[5] + g2c[6])

    class Ring:
        def __init__(self, low, count):
            self.low, self.count = low, count
            self.up, self.down = [], []

        def piece(self, there):
            half, start = window(there)
            return g2.at[pl.ds(self.low, self.count), half, pl.ds(start, WIN)]

        def slot(self, i):
            return zr.at[i, pl.ds(self.low, self.count)]

        def step(self, i):
            for s, far, copies, base in ((1, 4, self.up, 0), (-1, 3, self.down, 4)):
                if i >= far:
                    continue
                piece = self.piece(z + s * (far - i))
                if i:
                    copies[i - 1].wait_recv()
                    held = self.slot(base + i - 1)
                    held[...] = held[...] + piece[...]
                    piece = held
                copies.append(send(piece, self.slot(base + i), at_z(z + s)))

        def end(self, units):
            self.up[3].wait_recv()
            self.down[2].wait_recv()
            total = self.piece(z)[...] + self.slot(3)[...] + self.slot(6)[...]
            for n, unit in enumerate(units):
                fin[core, unit] = total[n]

    ring_ab, ring_d = Ring(0, 2), Ring(2, 1)

    weight_sent = []

    def weights(stage):
        spans = ((), (1, 2, 3), (1, 2, 3), tuple(range(1, 8)))
        if stage == 0:
            swap_weight.wait_recv()
            wt[2] = wt[0] + wt[1]
        else:
            for copy in weight_sent:
                copy.wait_recv()
            weight_sent.clear()
            value = wt[1 + stage]
            low = (0, 3, 6)[stage - 1]
            for n in range(len(spans[stage])):
                value = value + wx[low + n]
            wt[2 + stage] = value
        if stage < 3:
            low = (0, 3, 6)[stage]
            for n, s in enumerate(spans[stage + 1]):
                device = at_z(z + s) if stage == 2 else at_axis(1 - stage, s)
                weight_sent.append(send(wt.at[2 + stage], wx.at[low + n], device))

    settle(A, 2)
    trees1[A].far()
    settle(B, 2)
    trees1[B].far()
    settle(C, 1)
    c_step(0)
    settle(A, 1)
    settle(A, -1)
    trees1[A].near()
    settle(B, 1)
    settle(B, -1)
    trees1[B].near()
    settle(C, 0)
    c_step(1)
    weights(0)
    c_step(2)
    trees1[A].relay()
    trees1[B].relay()
    settle(D, 2)
    trees1[D].far()
    settle(D, 1)
    settle(D, -1)
    trees1[D].near()
    weights(1)
    c_step(3)
    settle(A, 0)
    settle(B, 0)
    settle(D, 0)
    c_step(4)
    weights(2)
    c_step(5)
    c_step(6)
    for unit in (A, B):
        end_first(unit)
        trees2[unit].far()
        trees2[unit].near()
    trees1[D].relay()
    trees2[A].relay()
    trees2[B].relay()
    c_finish()
    tree_c.far()
    tree_c.near()
    end_second(A)
    end_second(B)
    ring_ab.step(0)
    tree_c.relay()
    ring_ab.step(1)
    end_first(D)
    trees2[D].far()
    trees2[D].near()
    c_second_end()
    ring_ab.step(2)
    trees2[D].relay()
    ring_ab.step(3)
    end_second(D)
    ring_d.step(0)
    ring_ab.end((A, B))
    ring_d.step(1)
    c_end()
    weights(3)
    early = len(sent) - 4
    ring_d.step(2)
    for copy in sent[:early]:
        copy.wait_send()
    ring_d.step(3)
    ring_d.end((D,))
    last = send(fin.at[core], fin.at[core], partner)
    last.wait_recv()
    total = wt[5]
    for odd in (0, 1):
        for c in (0, 1):
            @pl.when((lax.rem(zl, 2) == odd) & (core == c))
            def _():
                low = 4 * odd + 14 * c
                for p in (0, 1):
                    for unit in range(4):
                        out[p, :, unit * 128:(unit + 1) * 128] = fin[p, unit, low:low + 14] / total[:1]
    for copy in sent[early:]:
        copy.wait_send()
    assert len(sent) <= N_SEM


def merge(deltas, ages, table):
    vmem = lambda *shape: pltpu.VMEM(shape, F32)
    return pl.pallas_call(
        kernel,
        out_shape=jax.ShapeDtypeStruct((2, 14, 512), F32),
        in_specs=[
            pl.BlockSpec(memory_space=pl.ANY),
            pl.BlockSpec(memory_space=pltpu.SMEM),
            pl.BlockSpec(memory_space=pltpu.SMEM),
        ],
        out_specs=pl.BlockSpec(memory_space=pltpu.VMEM),
        scratch_shapes=[
            pltpu.VMEM((3584, 512), jnp.bfloat16),
            pltpu.VMEM((3584, 512), jnp.bfloat16),
            vmem(4, 32, BLOCK, 128),
            vmem(4, 32, BLOCK, 128),
            vmem(4, 32, BLOCK, 128),
            vmem(3, 3, 2, 4, BLOCK, 128),
            vmem(3, 3, 2, BLOCK, 128),
            vmem(2, 7, 8, WIN, 128),
            vmem(3, 2, 2, WIN, 128),
            vmem(7, 3, WIN, 128),
            vmem(3, 2, 4, BLOCK, 128),
            vmem(16, WIN, 128),
            vmem(3, 2, BLOCK, 128),
            vmem(7, WIN, 128),
            vmem(2, 4, WIN, 128),
            vmem(6, 8, 128),
            vmem(13, 8, 128),
            pltpu.SemaphoreType.DMA((N_SEM,)),
            pltpu.SemaphoreType.DMA((N_SEM,)),
            pltpu.SemaphoreType.DMA((2,)),
        ],
        compiler_params=pltpu.CompilerParams(
            collective_id=0, has_side_effects=True, vmem_limit_bytes=60 * 2**20),
        name="merge",
    )(deltas, ages, table)


def local(deltas, ages, table, params, momentum):
    merged = merge(deltas, ages, table)
    new_momentum = momentum_decay * momentum + merged
    new_params = params - outer_rate * (merged + momentum_decay * new_momentum)
    return (new_params, new_momentum)


def solution(mesh):
    torus = Mesh(mesh.devices.reshape(2, 4, 4, 4, 2), ROW_COL)
    in_specs = (
        P(ROW_COL, None, None, None),
        P(ROW, COL),
        P(),
        P(None, ROW_COL, None),
        P(None, ROW_COL, None),
    )
    out_specs = (P(None, ROW_COL, None), P(None, ROW_COL, None))
    return jax.shard_map(local, mesh=torus, in_specs=in_specs, out_specs=out_specs, check_vma=False)
```

```python
import jax
import jax.numpy as jnp
from jax import lax
from jax.experimental import pallas as pl
from jax.experimental.pallas import tpu as pltpu
from jax.sharding import Mesh
from jax.sharding import PartitionSpec as P

ROW = ("z_hi", "y", "x")
COL = ("z_lo", "core")
ROW_COL = ROW + COL
MESH = pl.DeviceIdType.MESH
F32 = jnp.float32

momentum_decay = 0.9
outer_rate = 0.7

BLOCK = 112
WIN = 32
N_SEND, N_RECV = 13, 55
X, Y, ZX, ZY = "X", "Y", "ZX", "ZY"
KINDS = ((X, Y, ZX, ZY), (X, Y, X, Y))

ORDERS = (
    ((2, 1, 0), (0, 2), (2, 1, 1), (1, 2), (3, 1, 0), (3, 1, 1), (2, 0, 0), (2, 0, 1),
     (0, 1), (0, -1), (3, 0, 0), (3, 0, 1), (1, 1), (1, -1), (0, 0), (1, 0)),
    ((0, 2), (1, 2), (0, 1), (0, -1), (1, 1), (1, -1), (2, 2), (3, 2),
     (2, 1), (2, -1), (3, 1), (3, -1), (0, 0), (1, 0), (2, 0), (3, 0)),
)
AHEAD = 4


def wrap4(value):
    return lax.rem(value + 4, 4)


def kernel(delta, ages, table, out, age, levels, theirs, ours, give, got, mine, t1, t2, tc, u2, zr,
           g1, g1c, g2, g2c, fin, wt, wx, send_sems, recv_sems, swap_send, swap_recv, load_sems):
    zh, y, x, zl, core = [lax.axis_index(name) for name in ROW_COL]
    z = zh * 4 + zl
    barrier = pltpu.get_barrier_semaphore()

    load_age = pltpu.make_async_copy(ages, age, load_sems.at[5])
    load_levels = pltpu.make_async_copy(table, levels, load_sems.at[6])
    load_age.start()
    load_levels.start()

    def program(me):
        kinds, other_kinds = KINDS[me], KINDS[1 - me]
        order, other_order = ORDERS[me], ORDERS[1 - me]

        def load(source, target, unit, sem):
            lanes = pl.ds(unit * 128, 128)
            return pltpu.make_async_copy(delta.at[0, source, :, lanes], target.at[:, lanes], load_sems.at[sem])

        first_use = list(dict.fromkeys(unit for unit, *_ in other_order))
        load_theirs = {unit: load(1 - me, theirs, unit, unit) for unit in first_use}
        load_ours = pltpu.make_async_copy(delta.at[0, me], ours, load_sems.at[4])
        for unit in first_use:
            load_theirs[unit].start()

        def at_z(there):
            there = lax.rem(there + 16, 8)
            return (there // 4, y, x, lax.rem(there, 4), me)

        def at_axis(axis, step):
            if axis == X:
                return (zh, y, wrap4(x + step), zl, me)
            return (zh, wrap4(y + step), x, zl, me)

        partner = (zh, y, x, zl, 1 - me)
        peers = [partner]
        peers += [at_axis(axis, s) for axis in (X, Y) for s in (1, 2, 3)]
        peers += [at_z(z + s) for s in range(1, 8)]
        for peer in peers:
            pl.semaphore_signal(barrier, inc=1, device_id=peer, device_id_type=MESH)
        load_age.wait()
        load_levels.wait()
        weight = levels[age[0, 0]]
        wt[0] = jnp.full((8, 128), weight, F32)

        def copy_to(device, src, dst, send_sem, recv_sem):
            return pltpu.make_async_remote_copy(
                src_ref=src, dst_ref=dst, send_sem=send_sem, recv_sem=recv_sem,
                device_id=device, device_id_type=MESH)

        groups, recvs = [], []

        def new_recv():
            recvs.append(len(recvs))
            return recv_sems.at[recvs[-1]]

        class Group:
            def __init__(self, whole):
                self.whole, self.send_sem = whole, send_sems.at[len(groups)]
                groups.append(self)

            def send(self, src, dst, device, recv_sem):
                copy = copy_to(device, src, dst, self.send_sem, recv_sem)
                copy.start()
                return copy

            def drain(self):
                copy_to(partner, self.whole, self.whole, self.send_sem, recv_sems.at[0]).wait_send()

        def arrived(whole, recv_sem):
            copy_to(partner, whole, whole, send_sems.at[0], recv_sem).wait_recv()

        def swap(src, dst, i):
            return copy_to(partner, src, dst, swap_send.at[max(i - 15, 0)], swap_recv.at[i])

        def position(axis):
            return x if axis == X else y

        def cross(axis):
            return Y if axis == X else X

        def term(src, unit, kind, slot):
            if kind in (ZX, ZY):
                half, d, j = slot // 16, lax.rem(slot, 16) // 4, lax.rem(slot, 4)
            else:
                d, half, j = slot // 8, lax.rem(slot, 8) // 4, lax.rem(slot, 4)
            block = half * 16 + (j * 4 + d if kind in (X, ZX) else d * 4 + j)
            start = pl.multiple_of(block * BLOCK, 16)
            return src[pl.ds(start, BLOCK), unit * 128:(unit + 1) * 128].astype(F32) * weight

        def chunk(kind, step):
            if kind in (ZX, ZY):
                return lax.rem(zh + step[0], 2) * 16 + 8 * step[1]
            return wrap4(position(kind) + step[0]) * 8

        gifts = []

        def put_together(n):
            unit, *step = other_order[n]
            kind = other_kinds[unit]
            if unit in load_theirs:
                load_theirs.pop(unit).wait()
            base = chunk(kind, step)

            @pl.loop(0, 8)
            def _(k):
                give[unit, base + k] = term(theirs, unit, kind, base + k)

            gifts.append(swap(give.at[unit, pl.ds(base, 8)], got.at[unit, pl.ds(base, 8)], n))

        def settle(n):
            unit, *step = order[n]
            kind = kinds[unit]
            base = chunk(kind, step)
            swap(got.at[unit, pl.ds(base, 8)], got.at[unit, pl.ds(base, 8)], n).wait_recv()

            @pl.loop(0, 8)
            def _(k):
                mine[unit, base + k] = got[unit, base + k] + term(ours, unit, kind, base + k)

            if n + AHEAD < 16:
                put_together(n + AHEAD)
                gifts[-1].start()

        class Tree:
            def __init__(self, piece, slots, axis):
                self.piece, self.slots, self.axis, self.at = piece, slots, axis, position(axis)
                self.group = Group(slots)
                self.m0, self.first, self.rest = {}, {1: new_recv(), -1: new_recv()}, new_recv()

            def far(self):
                for s in (1, -1):
                    src = self.piece(int(s < 0), wrap4(self.at + 2))
                    dst = self.slots.at[0, int(s < 0)]
                    self.m0[s] = self.group.send(src, dst, at_axis(self.axis, s), self.first[s])

            def near(self):
                for s in (1, -1):
                    src = self.piece(int(s > 0), wrap4(self.at + s))
                    self.group.send(src, self.slots.at[1, int(s < 0)], at_axis(self.axis, s), self.rest)

            def relay(self):
                for s in (1, -1):
                    self.m0[s].wait_recv()
                    held = self.slots.at[0, int(s < 0)]
                    held[...] = held[...] + self.piece(int(s < 0), wrap4(self.at + s))[...]
                    self.group.send(held, self.slots.at[2, int(s < 0)], at_axis(self.axis, s), self.rest)

            def finish(self, put):
                arrived(self.slots.at[pl.ds(1, 2)], self.rest)
                for h in (0, 1):
                    put(h, self.piece(h, self.at)[...] + self.slots[2, h] + self.slots[1, 1 - h])

        def window(there):
            there = lax.rem(there + 16, 8)
            low = lax.rem(there, 4)
            return there // 4, pl.multiple_of((low // 2) * 56 + lax.rem(low, 2) * 24, 8)

        class Flat:
            def __init__(self, unit):
                axis = kinds[unit]
                self.unit = unit
                self.one = Tree(lambda h, d: mine.at[unit, pl.ds(d * 8 + h * 4, 4)], t1.at[unit], axis)
                self.two = Tree(lambda h, d: g1.at[unit, h, d], t2.at[unit], cross(axis))
                self.group, self.last, self.far_sem = Group(zr.at[unit]), new_recv(), new_recv()
                self.way = 1 if unit % 2 == 0 else -1

            def end_one(self):
                def put(h, value):
                    g1[self.unit, h] = value
                self.one.finish(put)
                self.two.far()
                self.two.near()

            def end_two(self):
                def put(h, value):
                    g2[self.unit, h] = value
                self.two.finish(put)
                self.send_z(4, 2 * self.way, 4, self.far_sem)
                for s in (1, -1):
                    self.send_z(3 * s, s, 5 + int(s < 0), self.far_sem)
                for s in (1, -1):
                    self.send_z(s, s, int(s < 0), self.last)

            def piece_z(self, there):
                half, start = window(there)
                return g2.at[self.unit, half, pl.ds(start, WIN)]

            def send_z(self, there, step, slot, sem):
                self.group.send(self.piece_z(z + there), zr.at[self.unit, slot], at_z(z + step), sem)

            def relay_z(self):
                arrived(zr.at[self.unit, pl.ds(4, 3)], self.far_sem)
                for s in (1, -1):
                    held = zr.at[self.unit, 5 + int(s < 0)]
                    value = held[...] + self.piece_z(z + 2 * s)[...]
                    if s == self.way:
                        value = value + zr[self.unit, 4]
                    held[...] = value
                    self.group.send(held, zr.at[self.unit, 2 + int(s < 0)], at_z(z + 2 * s), self.last)

            def end(self):
                arrived(zr.at[self.unit, pl.ds(0, 4)], self.last)
                value = self.piece_z(z)[...]
                for n in range(4):
                    value = value + zr[self.unit, n]
                fin[me, self.unit] = value

        class Deep:
            dist = (4, 3, 3, 2, 2, 1, 1)

            def __init__(self, unit):
                self.unit, self.n = unit, unit - 2
                self.axis = X if kinds[unit] == ZX else Y
                self.copies, self.ring = {}, Group(tc.at[self.n])
                self.two = Tree(lambda h, d: g1c.at[self.n, pl.ds(d * 4 + h * 2, 2)], u2.at[self.n], self.axis)
                self.group, self.last = Group(g2c.at[self.n, pl.ds(4, 3)]), new_recv()

            def piece(self, there, half):
                up, start = window(there)
                return mine.at[self.unit, pl.ds(up * 16 + half * 8, 8), pl.ds(start, WIN)]

            def step(self, i, ways=(1, -1)):
                for s in ways:
                    k = int(s < 0)
                    piece = self.piece(z + s * self.dist[i], k if i % 2 == 0 else 1 - k)
                    if i >= 2:
                        self.copies[s, i - 2].wait_recv()
                        held = tc.at[self.n, k, i - 2]
                        held[...] = held[...] + piece[...]
                        piece = held
                    self.copies[s, i] = self.ring.send(piece, tc.at[self.n, k, i], at_z(z + s), new_recv())

            def end_one(self):
                for i in (5, 6):
                    for s in (1, -1):
                        self.copies[s, i].wait_recv()
                for half in (0, 1):
                    g1c[self.n, half * 8:half * 8 + 8] = (
                        self.piece(z, half)[...] + tc[self.n, half, 6] + tc[self.n, 1 - half, 5])
                self.two.far()
                self.two.near()

            def end_two(self):
                def put(h, value):
                    g2c[self.n, h * 2:h * 2 + 2] = value
                self.two.finish(put)
                axis = cross(self.axis)
                for s in (2, 1, 3):
                    src = g2c.at[self.n, wrap4(position(axis) + s)]
                    self.group.send(src, g2c.at[self.n, 3 + s], at_axis(axis, s), self.last)

            def end(self):
                arrived(g2c.at[self.n, pl.ds(4, 3)], self.last)
                fin[me, self.unit] = g2c[self.n, position(cross(self.axis))] + (
                    g2c[self.n, 4] + g2c[self.n, 5] + g2c[self.n, 6])

        weight_group, weight_sems = Group(wx), [new_recv() for _ in range(3)]

        def weights(stage):
            spans = ((), (1, 2, 3), (1, 2, 3), (4, 3, 5, 2, 6, 1, 7))
            lows = (0, 3, 6)
            if stage == 0:
                swap(wt.at[1], wt.at[1], 16).wait_recv()
                wt[2] = wt[0] + wt[1]
            else:
                low, count = lows[stage - 1], len(spans[stage])
                arrived(wx.at[pl.ds(low, count)], weight_sems[stage - 1])
                value = wt[1 + stage]
                for n in range(count):
                    value = value + wx[low + n]
                wt[2 + stage] = value
            if stage < 3:
                for n, s in enumerate(spans[stage + 1]):
                    device = at_z(z + s) if stage == 2 else at_axis((X, Y)[stage], s)
                    weight_group.send(wt.at[2 + stage], wx.at[lows[stage] + n], device, weight_sems[stage])

        put_together(0)
        load_ours.start()
        pl.semaphore_wait(barrier, len(peers))
        swap_weight = swap(wt.at[0], wt.at[1], 16)
        swap_weight.start()
        gifts[0].start()
        for n in range(1, AHEAD):
            put_together(n)
            gifts[n].start()
        weights(0)
        load_ours.wait()

        a, b = Flat(0), Flat(1)
        if me == 0:
            c, e = Deep(2), Deep(3)
            settle(0)
            c.step(0, (1,))
            settle(1)
            a.one.far()
            settle(2)
            c.step(0, (-1,))
            settle(3)
            b.one.far()
            settle(4)
            e.step(0, (1,))
            settle(5)
            e.step(0, (-1,))
            settle(6)
            settle(7)
            c.step(1)
            settle(8)
            settle(9)
            a.one.near()
            c.step(2)
            settle(10)
            settle(11)
            e.step(1)
            settle(12)
            settle(13)
            b.one.near()
            e.step(2)
            a.one.relay()
            settle(14)
            settle(15)
            b.one.relay()
            weights(1)
            for i in (3, 4):
                c.step(i)
                e.step(i)
            for i in (5, 6):
                c.step(i)
                e.step(i)
            a.end_one()
            b.end_one()
            c.end_one()
            e.end_one()
            weights(2)
            a.two.relay()
            b.two.relay()
            c.two.relay()
            e.two.relay()
            a.end_two()
            b.end_two()
            a.relay_z()
            b.relay_z()
            c.end_two()
            e.end_two()
        else:
            d, f = Flat(2), Flat(3)
            settle(0)
            a.one.far()
            settle(1)
            b.one.far()
            settle(2)
            settle(3)
            a.one.near()
            settle(4)
            settle(5)
            b.one.near()
            for n in range(6, 10):
                settle(n)
            d.one.far()
            d.one.near()
            for n in range(10, 12):
                settle(n)
            f.one.far()
            f.one.near()
            a.one.relay()
            b.one.relay()
            for n in range(12, 16):
                settle(n)
            weights(1)
            d.one.relay()
            f.one.relay()
            a.end_one()
            b.end_one()
            weights(2)
            d.end_one()
            f.end_one()
            a.two.relay()
            b.two.relay()
            d.two.relay()
            f.two.relay()
            a.end_two()
            b.end_two()
            d.end_two()
            f.end_two()
            a.relay_z()
            b.relay_z()
            d.relay_z()
            f.relay_z()
        a.end()
        b.end()
        first_swap = swap(fin.at[me, pl.ds(0, 2)], fin.at[me, pl.ds(0, 2)], 17)
        first_swap.start()
        copy_to(partner, give, give, swap_send.at[0], swap_recv.at[0]).wait_send()
        swap_weight.wait_send()
        weights(3)
        for unit in ((c, e) if me == 0 else (d, f)):
            unit.end()
        last_swap = swap(fin.at[me, pl.ds(2, 2)], fin.at[me, pl.ds(2, 2)], 18)
        last_swap.start()
        for group in groups:
            group.drain()
        assert len(groups) <= N_SEND and len(recvs) <= N_RECV
        for i in (17, 18):
            theirs_fin = fin.at[1 - me, pl.ds(2 * (i - 17), 2)]
            swap(theirs_fin, theirs_fin, i).wait_recv()
        total = wt[5]
        for odd in (0, 1):
            @pl.when(lax.rem(zl, 2) == odd)
            def _():
                low = 4 * odd + 14 * me
                for p in (0, 1):
                    for unit in range(4):
                        out[:, p, unit * 128:(unit + 1) * 128] = fin[p, unit, low:low + 14] / total[:1]
        first_swap.wait_send()
        last_swap.wait_send()

    for me in (0, 1):
        @pl.when(core == me)
        def _():
            program(me)


def merge(deltas, ages, table):
    vmem = lambda *shape: pltpu.VMEM(shape, F32)
    return pl.pallas_call(
        kernel,
        out_shape=pltpu.VMEM((14, 2, 512), F32),
        in_specs=[
            pl.BlockSpec(memory_space=pltpu.HBM),
            pl.BlockSpec(memory_space=pltpu.HBM),
            pl.BlockSpec(memory_space=pltpu.HBM),
        ],
        out_specs=pl.BlockSpec(memory_space=pltpu.VMEM),
        scratch_shapes=[
            pltpu.SMEM((1, 1), jnp.int32),
            pltpu.SMEM((8,), F32),
            pltpu.VMEM((3584, 512), jnp.bfloat16),
            pltpu.VMEM((3584, 512), jnp.bfloat16),
            vmem(4, 32, BLOCK, 128),
            vmem(4, 32, BLOCK, 128),
            vmem(4, 32, BLOCK, 128),
            vmem(4, 3, 2, 4, BLOCK, 128),
            vmem(4, 3, 2, BLOCK, 128),
            vmem(2, 2, 7, 8, WIN, 128),
            vmem(2, 3, 2, 2, WIN, 128),
            vmem(4, 7, WIN, 128),
            vmem(4, 2, 4, BLOCK, 128),
            vmem(2, 16, WIN, 128),
            vmem(4, 2, BLOCK, 128),
            vmem(2, 7, WIN, 128),
            vmem(2, 4, WIN, 128),
            vmem(6, 8, 128),
            vmem(13, 8, 128),
            pltpu.SemaphoreType.DMA((N_SEND,)),
            pltpu.SemaphoreType.DMA((N_RECV,)),
            pltpu.SemaphoreType.DMA((4,)),
            pltpu.SemaphoreType.DMA((19,)),
            pltpu.SemaphoreType.DMA((7,)),
        ],
        compiler_params=pltpu.CompilerParams(
            collective_id=0, has_side_effects=True, vmem_limit_bytes=60 * 2**20),
        name="merge",
    )(deltas, ages, table)


def local(deltas, ages, table, params, momentum):
    merged = jnp.transpose(merge(deltas, ages, table), (1, 0, 2))
    new_momentum = momentum_decay * momentum + merged
    new_params = params - outer_rate * (merged + momentum_decay * new_momentum)
    return (new_params, new_momentum)


def solution(mesh):
    torus = Mesh(mesh.devices.reshape(2, 4, 4, 4, 2), ROW_COL)
    in_specs = (
        P(ROW_COL, None, None, None),
        P(ROW, COL),
        P(),
        P(None, ROW_COL, None),
        P(None, ROW_COL, None),
    )
    out_specs = (P(None, ROW_COL, None), P(None, ROW_COL, None))
    return jax.shard_map(local, mesh=torus, in_specs=in_specs, out_specs=out_specs, check_vma=False)
```

```python
import jax
import jax.numpy as jnp
from jax import lax
from jax.experimental import pallas as pl
from jax.experimental.pallas import tpu as pltpu
from jax.sharding import Mesh
from jax.sharding import PartitionSpec as P

ROW = ("z_hi", "y", "x")
COL = ("z_lo", "core")
ROW_COL = ROW + COL
MESH = pl.DeviceIdType.MESH
F32 = jnp.float32

momentum_decay = 0.9
outer_rate = 0.7

BLOCK = 112
WIN = 32
N_SEND, N_RECV = 13, 76
X, Y, ZX, ZY = "X", "Y", "ZX", "ZY"
KINDS = ((X, Y, X, Y), (X, Y, ZX, ZY))

ORDERS = (
    ((0, 2), (1, 2), (0, 1), (0, -1), (1, 1), (1, -1), (2, 2), (3, 2),
     (2, 1), (2, -1), (3, 1), (3, -1), (0, 0), (1, 0), (2, 0), (3, 0)),
    ((2, 1, 0), (2, 1, 1), (3, 1, 0), (3, 1, 1), (2, 0, 0), (2, 0, 1), (3, 0, 0), (3, 0, 1),
     (0, 2), (1, 2), (0, 1), (0, -1), (1, 1), (1, -1), (0, 0), (1, 0)),
)
AHEAD = 4


def wrap4(value):
    return lax.rem(value + 4, 4)


def kernel(delta, ages, table, out, age, levels, theirs, ours, give, got, mine, t1, t2, tc, tz, u2, zr,
           g1, g1c, g2, g2c, g2m, fin, wt, wx, send_sems, recv_sems, swap_send, swap_recv, load_sems):
    zh, y, x, zl, core = [lax.axis_index(name) for name in ROW_COL]
    z = zh * 4 + zl
    barrier = pltpu.get_barrier_semaphore()

    load_age = pltpu.make_async_copy(ages, age, load_sems.at[5])
    load_levels = pltpu.make_async_copy(table, levels, load_sems.at[6])
    load_age.start()
    load_levels.start()

    def program(me):
        kinds, other_kinds = KINDS[me], KINDS[1 - me]
        order, other_order = ORDERS[me], ORDERS[1 - me]

        def load(source, target, unit, sem):
            lanes = pl.ds(unit * 128, 128)
            return pltpu.make_async_copy(delta.at[0, source, :, lanes], target.at[:, lanes], load_sems.at[sem])

        first_use = list(dict.fromkeys(unit for unit, *_ in other_order))
        load_theirs = {unit: load(1 - me, theirs, unit, unit) for unit in first_use}
        load_ours = pltpu.make_async_copy(delta.at[0, me], ours, load_sems.at[4])
        for unit in first_use:
            load_theirs[unit].start()

        def at_z(there):
            there = lax.rem(there + 16, 8)
            return (there // 4, y, x, lax.rem(there, 4), me)

        def at_axis(axis, step):
            if axis == X:
                return (zh, y, wrap4(x + step), zl, me)
            return (zh, wrap4(y + step), x, zl, me)

        partner = (zh, y, x, zl, 1 - me)
        peers = [partner]
        peers += [at_axis(axis, s) for axis in (X, Y) for s in (1, 2, 3)]
        peers += [at_z(z + s) for s in (1, -1, 2, -2)]
        for peer in peers:
            pl.semaphore_signal(barrier, inc=1, device_id=peer, device_id_type=MESH)
        load_age.wait()
        load_levels.wait()
        weight = levels[age[0]]
        wt[0] = jnp.full((8, 128), weight, F32)

        def copy_to(device, src, dst, send_sem, recv_sem):
            return pltpu.make_async_remote_copy(
                src_ref=src, dst_ref=dst, send_sem=send_sem, recv_sem=recv_sem,
                device_id=device, device_id_type=MESH)

        groups, recvs = [], []

        def new_recv():
            recvs.append(len(recvs))
            return recv_sems.at[recvs[-1]]

        class Group:
            def __init__(self, whole):
                self.whole, self.send_sem = whole, send_sems.at[len(groups)]
                groups.append(self)

            def send(self, src, dst, device, recv_sem):
                copy = copy_to(device, src, dst, self.send_sem, recv_sem)
                copy.start()
                return copy

            def drain(self):
                copy_to(partner, self.whole, self.whole, self.send_sem, recv_sems.at[0]).wait_send()

        def arrived(whole, recv_sem):
            copy_to(partner, whole, whole, send_sems.at[0], recv_sem).wait_recv()

        def swap(src, dst, i):
            return copy_to(partner, src, dst, swap_send.at[max(i - 15, 0)], swap_recv.at[i])

        def position(axis):
            return x if axis == X else y

        def cross(axis):
            return Y if axis == X else X

        def term(src, unit, kind, slot):
            if kind in (ZX, ZY):
                half, d, j = slot // 16, lax.rem(slot, 16) // 4, lax.rem(slot, 4)
            else:
                d, half, j = slot // 8, lax.rem(slot, 8) // 4, lax.rem(slot, 4)
            block = half * 16 + (j * 4 + d if kind in (X, ZX) else d * 4 + j)
            start = pl.multiple_of(block * BLOCK, 16)
            return src[pl.ds(start, BLOCK), unit * 128:(unit + 1) * 128].astype(F32) * weight

        def chunk(kind, step):
            if kind in (ZX, ZY):
                return lax.rem(zh + step[0], 2) * 16 + 8 * step[1]
            return wrap4(position(kind) + step[0]) * 8

        gifts = []

        def put_together(n):
            unit, *step = other_order[n]
            kind = other_kinds[unit]
            if unit in load_theirs:
                load_theirs.pop(unit).wait()
            base = chunk(kind, step)

            @pl.loop(0, 8)
            def _(k):
                give[unit, base + k] = term(theirs, unit, kind, base + k)

            gifts.append(swap(give.at[unit, pl.ds(base, 8)], got.at[unit, pl.ds(base, 8)], n))

        def settle(n):
            unit, *step = order[n]
            kind = kinds[unit]
            base = chunk(kind, step)
            swap(got.at[unit, pl.ds(base, 8)], got.at[unit, pl.ds(base, 8)], n).wait_recv()

            @pl.loop(0, 8)
            def _(k):
                mine[unit, base + k] = got[unit, base + k] + term(ours, unit, kind, base + k)

            if n + AHEAD < 16:
                put_together(n + AHEAD)
                gifts[-1].start()

        class Tree:
            def __init__(self, piece, slots, axis):
                self.piece, self.slots, self.axis, self.at = piece, slots, axis, position(axis)
                self.group = Group(slots)
                self.m0, self.first, self.rest = {}, {1: new_recv(), -1: new_recv()}, new_recv()

            def far(self):
                for s in (1, -1):
                    src = self.piece(int(s < 0), wrap4(self.at + 2))
                    dst = self.slots.at[0, int(s < 0)]
                    self.m0[s] = self.group.send(src, dst, at_axis(self.axis, s), self.first[s])

            def near(self):
                for s in (1, -1):
                    src = self.piece(int(s > 0), wrap4(self.at + s))
                    self.group.send(src, self.slots.at[1, int(s < 0)], at_axis(self.axis, s), self.rest)

            def relay(self):
                for s in (1, -1):
                    self.m0[s].wait_recv()
                    held = self.slots.at[0, int(s < 0)]
                    held[...] = held[...] + self.piece(int(s < 0), wrap4(self.at + s))[...]
                    self.group.send(held, self.slots.at[2, int(s < 0)], at_axis(self.axis, s), self.rest)

            def finish(self, put):
                arrived(self.slots.at[pl.ds(1, 2)], self.rest)
                for h in (0, 1):
                    put(h, self.piece(h, self.at)[...] + self.slots[2, h] + self.slots[1, 1 - h])

        def window(there):
            there = lax.rem(there + 16, 8)
            low = lax.rem(there, 4)
            return there // 4, pl.multiple_of((low // 2) * 56 + lax.rem(low, 2) * 24, 8)

        class Quarters(Tree):
            def __init__(self, piece, slots, axis):
                super().__init__(piece, slots, axis)
                self.beside = position(cross(axis))
                self.parts = {step: new_recv() for step in (2, 1, -1, 0)}

            def relay(self):
                for s in (1, -1):
                    k = int(s < 0)
                    self.m0[s].wait_recv()
                    held = self.slots.at[0, k]
                    held[...] = held[...] + self.piece(k, wrap4(self.at + s))[...]
                    for step, sem in self.parts.items():
                        j = wrap4(self.beside + step)
                        self.group.send(held.at[j], self.slots.at[2, k, j], at_axis(self.axis, s), sem)

            def part(self, step, put):
                if step == 2:
                    arrived(self.slots.at[1], self.rest)
                j = wrap4(self.beside + step)
                arrived(self.slots.at[2, :, j], self.parts[step])
                for h in (0, 1):
                    put(h, j, self.piece(h, self.at)[j] + self.slots[2, h, j] + self.slots[1, 1 - h, j])

        class Flat:
            def __init__(self, unit):
                axis = kinds[unit]
                self.unit = unit
                self.one = Quarters(lambda h, d: mine.at[unit, pl.ds(d * 8 + h * 4, 4)], t1.at[unit], axis)
                self.two = Tree(lambda h, d: g1.at[unit, h, d], t2.at[unit], cross(axis))
                self.group, self.last, self.far_sem = Group(zr.at[unit]), new_recv(), new_recv()
                self.way = 1 if unit % 2 == 0 else -1

            def part(self, n):
                def put(h, j, value):
                    g1[self.unit, h, j] = value
                for step in ((2,), (1, -1), (0,))[n]:
                    self.one.part(step, put)
                if n == 0:
                    self.two.far()
                elif n == 1:
                    self.two.near()

            def end_two(self):
                def put(h, value):
                    g2[self.unit, h] = value
                self.two.finish(put)
                self.send_z(4, 2 * self.way, 4, self.far_sem)
                for s in (1, -1):
                    self.send_z(3 * s, s, 5 + int(s < 0), self.far_sem)
                for s in (1, -1):
                    self.send_z(s, s, int(s < 0), self.last)

            def piece_z(self, there):
                half, start = window(there)
                return g2.at[self.unit, half, pl.ds(start, WIN)]

            def send_z(self, there, step, slot, sem):
                self.group.send(self.piece_z(z + there), zr.at[self.unit, slot], at_z(z + step), sem)

            def relay_z(self):
                arrived(zr.at[self.unit, pl.ds(4, 3)], self.far_sem)
                for s in (1, -1):
                    held = zr.at[self.unit, 5 + int(s < 0)]
                    value = held[...] + self.piece_z(z + 2 * s)[...]
                    if s == self.way:
                        value = value + zr[self.unit, 4]
                    held[...] = value
                    self.group.send(held, zr.at[self.unit, 2 + int(s < 0)], at_z(z + 2 * s), self.last)

            def end(self):
                arrived(zr.at[self.unit, pl.ds(0, 4)], self.last)
                value = self.piece_z(z)[...]
                for n in range(4):
                    value = value + zr[self.unit, n]
                fin[me, self.unit] = value

        class Ring:
            dist = (4, 3, 3, 2, 2, 1, 1)

            def __init__(self, piece, slots):
                self.piece, self.slots = piece, slots
                self.group, self.copies = Group(slots), {}

            def step(self, i, ways=(1, -1)):
                for s in ways:
                    k = int(s < 0)
                    piece = self.piece(z + s * self.dist[i], k if i % 2 == 0 else 1 - k)
                    if i >= 2:
                        self.copies[s, i - 2].wait_recv()
                        held = self.slots.at[k, i - 2]
                        held[...] = held[...] + piece[...]
                        piece = held
                    self.copies[s, i] = self.group.send(piece, self.slots.at[k, i], at_z(z + s), new_recv())

            def finish(self, put):
                for i in (5, 6):
                    for s in (1, -1):
                        self.copies[s, i].wait_recv()
                for half in (0, 1):
                    put(half, self.piece(z, half)[...] + self.slots[half, 6] + self.slots[1 - half, 5])

        class Direct:
            def __init__(self, held, axis, unit):
                self.held, self.axis, self.unit = held, axis, unit
                self.group, self.sem = Group(held.at[pl.ds(4, 3)]), new_recv()

            def start(self):
                for s in (2, 1, 3):
                    src = self.held.at[wrap4(position(self.axis) + s)]
                    self.group.send(src, self.held.at[3 + s], at_axis(self.axis, s), self.sem)

            def end(self):
                arrived(self.held.at[pl.ds(4, 3)], self.sem)
                own = self.held[position(self.axis)]
                fin[me, self.unit] = own + (self.held[4] + self.held[5] + self.held[6])

        class Deep:
            def __init__(self, unit):
                n = unit - 2
                axis = X if kinds[unit] == ZX else Y

                def piece(there, half):
                    up, start = window(there)
                    return mine.at[unit, pl.ds(up * 16 + half * 8, 8), pl.ds(start, WIN)]

                self.n, self.one = n, Ring(piece, tc.at[n])
                self.two = Tree(lambda h, d: g1c.at[n, pl.ds(d * 4 + h * 2, 2)], u2.at[n], axis)
                self.last = Direct(g2c.at[n], cross(axis), unit)
                self.step, self.end = self.one.step, self.last.end

            def end_one(self):
                def put(half, value):
                    g1c[self.n, half * 8:half * 8 + 8] = value
                self.one.finish(put)

            def end_two(self):
                def put(h, value):
                    g2c[self.n, h * 2:h * 2 + 2] = value
                self.two.finish(put)
                self.last.start()

        class Mixed:
            def __init__(self, unit):
                axis = kinds[unit]

                def piece(there, half):
                    up, start = window(there)
                    return g1.at[unit, up, pl.ds(half * 2, 2), pl.ds(start, WIN)]

                self.unit = unit
                self.one = Tree(lambda h, d: mine.at[unit, pl.ds(d * 8 + h * 4, 4)], t1.at[unit], axis)
                self.two = Ring(piece, tz.at[unit])
                self.last = Direct(g2m.at[unit], cross(axis), unit)
                self.step, self.end = self.two.step, self.last.end

            def end_one(self):
                def put(h, value):
                    g1[self.unit, h] = value
                self.one.finish(put)

            def end_two(self):
                def put(half, value):
                    g2m[self.unit, half * 2:half * 2 + 2] = value
                self.two.finish(put)
                self.last.start()

        weight_group, weight_sems = Group(wx), [new_recv() for _ in range(4)]

        def spread(value, slots, devices, stage):
            wt[2 + stage] = value
            for slot, device in zip(slots, devices):
                weight_group.send(wt.at[2 + stage], wx.at[slot], device, weight_sems[stage])

        def weights(stage):
            if stage == 0:
                swap(wt.at[1], wt.at[1], 16).wait_recv()
                return spread(wt[0] + wt[1], (0, 1, 2), [at_axis(X, s) for s in (1, 2, 3)], 0)
            low, count = ((0, 3), (3, 3), (6, 4), (10, 2))[stage - 1]
            arrived(wx.at[pl.ds(low, count)], weight_sems[stage - 1])
            if stage == 1:
                spread(wt[2] + wx[0] + wx[1] + wx[2], (3, 4, 5), [at_axis(Y, s) for s in (1, 2, 3)], 1)
            elif stage == 2:
                spread(wt[3] + wx[3] + wx[4] + wx[5], (6, 7, 8, 9), [at_z(z + s) for s in (-1, 1, -2, 2)], 2)
            elif stage == 3:
                wt[5] = wx[6] + wx[8]
                weight_group.send(wt.at[5], wx.at[10], at_z(z - 2), weight_sems[3])
                weight_group.send(wx.at[7], wx.at[11], at_z(z + 2), weight_sems[3])
            else:
                wt[6] = wt[4] + (wx[6] + wx[7] + wx[8] + wx[9]) + (wx[10] + wx[11])

        put_together(0)
        load_ours.start()
        pl.semaphore_wait(barrier, len(peers))
        swap_weight = swap(wt.at[0], wt.at[1], 16)
        swap_weight.start()
        gifts[0].start()
        for n in range(1, AHEAD):
            put_together(n)
            gifts[n].start()
        weights(0)
        load_ours.wait()

        def hand_over(low, i):
            part = fin.at[me, pl.ds(low, 2)]
            copy = swap(part, part, i)
            copy.start()
            return copy

        if me == 0:
            a, b, d, f = Mixed(0), Mixed(1), Flat(2), Flat(3)
            settle(0)
            a.one.far()
            settle(1)
            b.one.far()
            settle(2)
            settle(3)
            a.one.near()
            settle(4)
            settle(5)
            b.one.near()
            settle(6)
            settle(7)
            settle(8)
            settle(9)
            weights(1)
            a.one.relay()
            d.one.far()
            d.one.near()
            b.one.relay()
            f.one.far()
            settle(10)
            settle(11)
            f.one.near()
            settle(12)
            settle(13)
            settle(14)
            settle(15)
            a.end_one()
            a.step(0)
            a.step(1)
            b.end_one()
            b.step(0)
            b.step(1)
            d.one.relay()
            f.one.relay()
            weights(2)
            a.step(2)
            a.step(3)
            b.step(2)
            b.step(3)
            a.step(4)
            a.step(5)
            b.step(4)
            b.step(5)
            weights(3)
            d.part(0)
            f.part(0)
            a.step(6)
            b.step(6)
            d.part(1)
            f.part(1)
            d.part(2)
            f.part(2)
            d.two.relay()
            f.two.relay()
            d.end_two()
            f.end_two()
            a.end_two()
            b.end_two()
            d.relay_z()
            f.relay_z()
            a.end()
            b.end()
            first_swap = hand_over(0, 17)
            d.end()
            f.end()
            last_swap = hand_over(2, 18)
        else:
            a, b, c, e = Flat(0), Flat(1), Deep(2), Deep(3)
            settle(0)
            c.step(0, (1,))
            settle(1)
            c.step(0, (-1,))
            settle(2)
            e.step(0, (1,))
            settle(3)
            e.step(0, (-1,))
            settle(4)
            settle(5)
            c.step(1)
            c.step(2)
            settle(6)
            settle(7)
            e.step(1)
            e.step(2)
            weights(1)
            settle(8)
            settle(9)
            c.step(3)
            settle(10)
            settle(11)
            settle(12)
            c.step(4)
            settle(13)
            settle(14)
            e.step(3)
            settle(15)
            e.step(4)
            c.step(5)
            a.one.far()
            b.one.far()
            a.one.near()
            b.one.near()
            e.step(5)
            c.step(6)
            a.one.relay()
            b.one.relay()
            e.step(6)
            weights(2)
            a.part(0)
            b.part(0)
            a.part(1)
            b.part(1)
            a.part(2)
            b.part(2)
            c.end_one()
            c.two.far()
            c.two.near()
            a.two.relay()
            b.two.relay()
            weights(3)
            e.end_one()
            e.two.far()
            e.two.near()
            a.end_two()
            b.end_two()
            c.two.relay()
            e.two.relay()
            a.relay_z()
            b.relay_z()
            c.end_two()
            e.end_two()
            a.end()
            b.end()
            first_swap = hand_over(0, 17)
            c.end()
            e.end()
            last_swap = hand_over(2, 18)
        copy_to(partner, give, give, swap_send.at[0], swap_recv.at[0]).wait_send()
        swap_weight.wait_send()
        weights(4)
        for group in groups:
            group.drain()
        assert len(groups) <= N_SEND and len(recvs) <= N_RECV
        for i in (17, 18):
            theirs_fin = fin.at[1 - me, pl.ds(2 * (i - 17), 2)]
            swap(theirs_fin, theirs_fin, i).wait_recv()
        total = wt[6]
        for odd in (0, 1):
            @pl.when(lax.rem(zl, 2) == odd)
            def _():
                low = 4 * odd + 14 * me
                for p in (0, 1):
                    for unit in range(4):
                        out[:, p, unit * 128:(unit + 1) * 128] = fin[p, unit, low:low + 14] / total[:1]
        first_swap.wait_send()
        last_swap.wait_send()

    for me in (0, 1):
        @pl.when(core == me)
        def _():
            program(me)


def merge(deltas, ages, table):
    vmem = lambda *shape: pltpu.VMEM(shape, F32)
    return pl.pallas_call(
        kernel,
        out_shape=pltpu.VMEM((14, 2, 512), F32),
        in_specs=[
            pl.BlockSpec(memory_space=pltpu.HBM),
            pl.BlockSpec(memory_space=pltpu.HBM),
            pl.BlockSpec(memory_space=pltpu.HBM),
        ],
        out_specs=pl.BlockSpec(memory_space=pltpu.VMEM),
        scratch_shapes=[
            pltpu.SMEM((1,), jnp.int32),
            pltpu.SMEM((8,), F32),
            pltpu.VMEM((3584, 512), jnp.bfloat16),
            pltpu.VMEM((3584, 512), jnp.bfloat16),
            vmem(4, 32, BLOCK, 128),
            vmem(4, 32, BLOCK, 128),
            vmem(4, 32, BLOCK, 128),
            vmem(4, 3, 2, 4, BLOCK, 128),
            vmem(4, 3, 2, BLOCK, 128),
            vmem(2, 2, 7, 8, WIN, 128),
            vmem(2, 2, 7, 2, WIN, 128),
            vmem(2, 3, 2, 2, WIN, 128),
            vmem(4, 7, WIN, 128),
            vmem(4, 2, 4, BLOCK, 128),
            vmem(2, 16, WIN, 128),
            vmem(4, 2, BLOCK, 128),
            vmem(2, 7, WIN, 128),
            vmem(2, 7, WIN, 128),
            vmem(2, 4, WIN, 128),
            vmem(7, 8, 128),
            vmem(12, 8, 128),
            pltpu.SemaphoreType.DMA((N_SEND,)),
            pltpu.SemaphoreType.DMA((N_RECV,)),
            pltpu.SemaphoreType.DMA((4,)),
            pltpu.SemaphoreType.DMA((19,)),
            pltpu.SemaphoreType.DMA((7,)),
        ],
        compiler_params=pltpu.CompilerParams(
            collective_id=0, has_side_effects=True, vmem_limit_bytes=60 * 2**20),
        name="merge",
    )(deltas, ages.reshape(1), table)


def local(deltas, ages, table, params, momentum):
    merged = jnp.transpose(merge(deltas, ages, table), (1, 0, 2))
    new_momentum = momentum_decay * momentum + merged
    new_params = params - outer_rate * (merged + momentum_decay * new_momentum)
    return (new_params, new_momentum)


def solution(mesh):
    torus = Mesh(mesh.devices.reshape(2, 4, 4, 4, 2), ROW_COL)
    in_specs = (
        P(ROW_COL, None, None, None),
        P(ROW, COL),
        P(),
        P(None, ROW_COL, None),
        P(None, ROW_COL, None),
    )
    out_specs = (P(None, ROW_COL, None), P(None, ROW_COL, None))
    return jax.shard_map(local, mesh=torus, in_specs=in_specs, out_specs=out_specs, check_vma=False)
```

```python
import jax
import jax.numpy as jnp
from jax import lax
from jax.experimental import pallas as pl
from jax.experimental.pallas import tpu as pltpu
from jax.sharding import Mesh
from jax.sharding import PartitionSpec as P

ROW = ("z_hi", "y", "x")
COL = ("z_lo", "core")
ROW_COL = ROW + COL
MESH = pl.DeviceIdType.MESH
F32 = jnp.float32

momentum_decay = 0.9
outer_rate = 0.7

BLOCK = 112
WIN = 32
N_SEND, N_RECV = 13, 44
X, Y, ZX, ZY = "X", "Y", "ZX", "ZY"
KINDS = ((X, Y, X, Y), (X, Y, ZX, ZY))

ORDERS = (
    ((0, 2), (1, 2), (0, 1), (0, -1), (1, 1), (1, -1), (2, 2), (3, 2),
     (2, 1), (2, -1), (3, 1), (3, -1), (0, 0), (1, 0), (2, 0), (3, 0)),
    ((2, 1, 0), (2, 1, 1), (3, 1, 0), (3, 1, 1), (2, 0, 0), (2, 0, 1), (3, 0, 0), (3, 0, 1),
     (0, 2), (1, 2), (0, 1), (0, -1), (1, 1), (1, -1), (0, 0), (1, 0)),
)
AHEAD = 4


def wrap4(value):
    return lax.rem(value + 4, 4)


def kernel(delta, ages, table, out, age, levels, theirs, ours, give, got, mine, t1, t2, tc, tz, u2, zr,
           g1, g1c, g2, g2c, g2m, fin, wt, wx, send_sems, recv_sems, swap_send, swap_recv, load_sems):
    zh, y, x, zl, core = [lax.axis_index(name) for name in ROW_COL]
    z = zh * 4 + zl
    barrier = pltpu.get_barrier_semaphore()

    load_age = pltpu.make_async_copy(ages, age, load_sems.at[5])
    load_levels = pltpu.make_async_copy(table, levels, load_sems.at[6])
    load_age.start()
    load_levels.start()

    def program(me):
        kinds, other_kinds = KINDS[me], KINDS[1 - me]
        order, other_order = ORDERS[me], ORDERS[1 - me]

        def load(source, target, unit, sem):
            lanes = pl.ds(unit * 128, 128)
            return pltpu.make_async_copy(delta.at[0, source, :, lanes], target.at[:, lanes], load_sems.at[sem])

        first_use = list(dict.fromkeys(unit for unit, *_ in other_order))
        load_theirs = {unit: load(1 - me, theirs, unit, unit) for unit in first_use}
        load_ours = pltpu.make_async_copy(delta.at[0, me], ours, load_sems.at[4])
        for unit in first_use:
            load_theirs[unit].start()

        def at_z(there):
            there = lax.rem(there + 16, 8)
            return (there // 4, y, x, lax.rem(there, 4), me)

        def at_axis(axis, step):
            if axis == X:
                return (zh, y, wrap4(x + step), zl, me)
            return (zh, wrap4(y + step), x, zl, me)

        partner = (zh, y, x, zl, 1 - me)
        peers = [partner]
        peers += [at_axis(axis, s) for axis in (X, Y) for s in (1, 2, 3)]
        peers += [at_z(z + s) for s in (1, -1, 2, -2)]
        for peer in peers:
            pl.semaphore_signal(barrier, inc=1, device_id=peer, device_id_type=MESH)
        load_age.wait()
        load_levels.wait()
        weight = levels[age[0]]
        wt[0] = jnp.full((8, 128), weight, F32)

        def copy_to(device, src, dst, send_sem, recv_sem):
            return pltpu.make_async_remote_copy(
                src_ref=src, dst_ref=dst, send_sem=send_sem, recv_sem=recv_sem,
                device_id=device, device_id_type=MESH)

        groups, recvs = [], []

        def new_recv():
            recvs.append(len(recvs))
            return recv_sems.at[recvs[-1]]

        class Group:
            def __init__(self, whole):
                self.whole, self.send_sem = whole, send_sems.at[len(groups)]
                groups.append(self)

            def send(self, src, dst, device, recv_sem):
                copy = copy_to(device, src, dst, self.send_sem, recv_sem)
                copy.start()
                return copy

            def drain(self):
                copy_to(partner, self.whole, self.whole, self.send_sem, recv_sems.at[0]).wait_send()

        def arrived(whole, recv_sem):
            copy_to(partner, whole, whole, send_sems.at[0], recv_sem).wait_recv()

        def swap(src, dst, i):
            return copy_to(partner, src, dst, swap_send.at[max(i - 15, 0)], swap_recv.at[i])

        def position(axis):
            return x if axis == X else y

        def cross(axis):
            return Y if axis == X else X

        def term(src, unit, kind, slot):
            if kind in (ZX, ZY):
                half, d, j = slot // 16, lax.rem(slot, 16) // 4, lax.rem(slot, 4)
            else:
                d, half, j = slot // 8, lax.rem(slot, 8) // 4, lax.rem(slot, 4)
            block = half * 16 + (j * 4 + d if kind in (X, ZX) else d * 4 + j)
            start = pl.multiple_of(block * BLOCK, 16)
            return src[pl.ds(start, BLOCK), unit * 128:(unit + 1) * 128].astype(F32) * weight

        def chunk(kind, step):
            if kind in (ZX, ZY):
                return lax.rem(zh + step[0], 2) * 16 + 8 * step[1]
            return wrap4(position(kind) + step[0]) * 8

        gifts = []

        def put_together(n):
            unit, *step = other_order[n]
            kind = other_kinds[unit]
            if unit in load_theirs:
                load_theirs.pop(unit).wait()
            base = chunk(kind, step)

            @pl.loop(0, 8)
            def _(k):
                give[unit, base + k] = term(theirs, unit, kind, base + k)

            gifts.append(swap(give.at[unit, pl.ds(base, 8)], got.at[unit, pl.ds(base, 8)], n))

        def settle(n):
            if n + AHEAD < 16:
                put_together(n + AHEAD)
                gifts[-1].start()
            unit, *step = order[n]
            kind = kinds[unit]
            base = chunk(kind, step)
            swap(got.at[unit, pl.ds(base, 8)], got.at[unit, pl.ds(base, 8)], n).wait_recv()

            @pl.loop(0, 8)
            def _(k):
                mine[unit, base + k] = got[unit, base + k] + term(ours, unit, kind, base + k)

        class Tree:
            def __init__(self, piece, slots, axis):
                self.piece, self.slots, self.axis, self.at = piece, slots, axis, position(axis)
                self.group = Group(slots)
                self.first, self.rest = new_recv(), new_recv()

            def far(self):
                for s in (1, -1):
                    src = self.piece(int(s < 0), wrap4(self.at + 2))
                    dst = self.slots.at[0, int(s < 0)]
                    self.group.send(src, dst, at_axis(self.axis, s), self.first)

            def near(self):
                for s in (1, -1):
                    src = self.piece(int(s > 0), wrap4(self.at + s))
                    self.group.send(src, self.slots.at[1, int(s < 0)], at_axis(self.axis, s), self.rest)

            def relay(self):
                arrived(self.slots.at[0], self.first)
                for s in (1, -1):
                    held = self.slots.at[0, int(s < 0)]
                    held[...] = held[...] + self.piece(int(s < 0), wrap4(self.at + s))[...]
                    self.group.send(held, self.slots.at[2, int(s < 0)], at_axis(self.axis, s), self.rest)

            def finish(self, put):
                arrived(self.slots.at[pl.ds(1, 2)], self.rest)
                for h in (0, 1):
                    put(h, self.piece(h, self.at)[...] + self.slots[2, h] + self.slots[1, 1 - h])

        def window(there):
            there = lax.rem(there + 16, 8)
            low = lax.rem(there, 4)
            return there // 4, pl.multiple_of((low // 2) * 56 + lax.rem(low, 2) * 24, 8)

        class Quarters(Tree):
            def __init__(self, piece, slots, axis):
                super().__init__(piece, slots, axis)
                self.beside = position(cross(axis))
                self.parts = {step: new_recv() for step in (2, 1, -1, 0)}

            def relay(self):
                arrived(self.slots.at[0], self.first)
                for s in (1, -1):
                    k = int(s < 0)
                    held = self.slots.at[0, k]
                    held[...] = held[...] + self.piece(k, wrap4(self.at + s))[...]
                    for step, sem in self.parts.items():
                        j = wrap4(self.beside + step)
                        self.group.send(held.at[j], self.slots.at[2, k, j], at_axis(self.axis, s), sem)

            def part(self, step, put):
                if step == 2:
                    arrived(self.slots.at[1], self.rest)
                j = wrap4(self.beside + step)
                arrived(self.slots.at[2, :, j], self.parts[step])
                for h in (0, 1):
                    put(h, j, self.piece(h, self.at)[j] + self.slots[2, h, j] + self.slots[1, 1 - h, j])

        class Flat:
            def __init__(self, unit):
                axis = kinds[unit]
                self.unit = unit
                self.one = Quarters(lambda h, d: mine.at[unit, pl.ds(d * 8 + h * 4, 4)], t1.at[unit], axis)
                self.two = Tree(lambda h, d: g1.at[unit, h, d], t2.at[unit], cross(axis))
                self.group, self.last, self.far_sem = Group(zr.at[unit]), new_recv(), new_recv()
                self.way = 1 if unit % 2 == 0 else -1

            def part(self, n):
                def put(h, j, value):
                    g1[self.unit, h, j] = value
                for step in ((2,), (1, -1), (0,))[n]:
                    self.one.part(step, put)
                if n == 0:
                    self.two.far()
                elif n == 1:
                    self.two.near()

            def end_two(self):
                def put(h, value):
                    g2[self.unit, h] = value
                self.two.finish(put)
                self.send_z(4, 2 * self.way, 4, self.far_sem)
                for s in (1, -1):
                    self.send_z(3 * s, s, 5 + int(s < 0), self.far_sem)
                for s in (1, -1):
                    self.send_z(s, s, int(s < 0), self.last)

            def piece_z(self, there):
                half, start = window(there)
                return g2.at[self.unit, half, pl.ds(start, WIN)]

            def send_z(self, there, step, slot, sem):
                self.group.send(self.piece_z(z + there), zr.at[self.unit, slot], at_z(z + step), sem)

            def relay_z(self):
                arrived(zr.at[self.unit, pl.ds(4, 3)], self.far_sem)
                for s in (1, -1):
                    held = zr.at[self.unit, 5 + int(s < 0)]
                    value = held[...] + self.piece_z(z + 2 * s)[...]
                    if s == self.way:
                        value = value + zr[self.unit, 4]
                    held[...] = value
                    self.group.send(held, zr.at[self.unit, 2 + int(s < 0)], at_z(z + 2 * s), self.last)

            def end(self):
                arrived(zr.at[self.unit, pl.ds(0, 4)], self.last)
                value = self.piece_z(z)[...]
                for n in range(4):
                    value = value + zr[self.unit, n]
                fin[me, self.unit] = value

        class Ring:
            dist = (4, 3, 3, 2, 2, 1, 1)

            def __init__(self, piece, slots):
                self.piece, self.slots = piece, slots
                self.group, self.sems = Group(slots), [new_recv() for _ in self.dist]

            def step(self, i, ways=(1, -1)):
                if i >= 2:
                    arrived(self.slots.at[:, i - 2], self.sems[i - 2])
                for s in ways:
                    k = int(s < 0)
                    piece = self.piece(z + s * self.dist[i], k if i % 2 == 0 else 1 - k)
                    if i >= 2:
                        held = self.slots.at[k, i - 2]
                        held[...] = held[...] + piece[...]
                        piece = held
                    self.group.send(piece, self.slots.at[k, i], at_z(z + s), self.sems[i])

            def finish(self, put):
                for i in (5, 6):
                    arrived(self.slots.at[:, i], self.sems[i])
                for half in (0, 1):
                    put(half, self.piece(z, half)[...] + self.slots[half, 6] + self.slots[1 - half, 5])

        class Direct:
            def __init__(self, held, axis, unit):
                self.held, self.axis, self.unit = held, axis, unit
                self.group, self.sem = Group(held.at[pl.ds(4, 3)]), new_recv()

            def start(self):
                for s in (2, 1, 3):
                    src = self.held.at[wrap4(position(self.axis) + s)]
                    self.group.send(src, self.held.at[3 + s], at_axis(self.axis, s), self.sem)

            def end(self):
                arrived(self.held.at[pl.ds(4, 3)], self.sem)
                own = self.held[position(self.axis)]
                fin[me, self.unit] = own + (self.held[4] + self.held[5] + self.held[6])

        class Deep:
            def __init__(self, unit):
                n = unit - 2
                axis = X if kinds[unit] == ZX else Y

                def piece(there, half):
                    up, start = window(there)
                    return mine.at[unit, pl.ds(up * 16 + half * 8, 8), pl.ds(start, WIN)]

                self.n, self.one = n, Ring(piece, tc.at[n])
                self.two = Tree(lambda h, d: g1c.at[n, pl.ds(d * 4 + h * 2, 2)], u2.at[n], axis)
                self.last = Direct(g2c.at[n], cross(axis), unit)
                self.step, self.end = self.one.step, self.last.end

            def end_one(self):
                def put(half, value):
                    g1c[self.n, half * 8:half * 8 + 8] = value
                self.one.finish(put)

            def end_two(self):
                def put(h, value):
                    g2c[self.n, h * 2:h * 2 + 2] = value
                self.two.finish(put)
                self.last.start()

        class Mixed:
            def __init__(self, unit):
                axis = kinds[unit]

                def piece(there, half):
                    up, start = window(there)
                    return g1.at[unit, up, pl.ds(half * 2, 2), pl.ds(start, WIN)]

                self.unit = unit
                self.one = Tree(lambda h, d: mine.at[unit, pl.ds(d * 8 + h * 4, 4)], t1.at[unit], axis)
                self.two = Ring(piece, tz.at[unit])
                self.last = Direct(g2m.at[unit], cross(axis), unit)
                self.step, self.end = self.two.step, self.last.end

            def end_one(self):
                def put(h, value):
                    g1[self.unit, h] = value
                self.one.finish(put)

            def end_two(self):
                def put(half, value):
                    g2m[self.unit, half * 2:half * 2 + 2] = value
                self.two.finish(put)
                self.last.start()

        weight_group, weight_sems = Group(wx), [new_recv() for _ in range(4)]

        def spread(value, slots, devices, stage):
            wt[2 + stage] = value
            for slot, device in zip(slots, devices):
                weight_group.send(wt.at[2 + stage], wx.at[slot], device, weight_sems[stage])

        def weights(stage):
            if stage == 0:
                swap(wt.at[1], wt.at[1], 16).wait_recv()
                return spread(wt[0] + wt[1], (0, 1, 2), [at_axis(X, s) for s in (1, 2, 3)], 0)
            low, count = ((0, 3), (3, 3), (6, 4), (10, 2))[stage - 1]
            arrived(wx.at[pl.ds(low, count)], weight_sems[stage - 1])
            if stage == 1:
                spread(wt[2] + wx[0] + wx[1] + wx[2], (3, 4, 5), [at_axis(Y, s) for s in (1, 2, 3)], 1)
            elif stage == 2:
                spread(wt[3] + wx[3] + wx[4] + wx[5], (6, 7, 8, 9), [at_z(z + s) for s in (-1, 1, -2, 2)], 2)
            elif stage == 3:
                wt[5] = wx[6] + wx[8]
                weight_group.send(wt.at[5], wx.at[10], at_z(z - 2), weight_sems[3])
                weight_group.send(wx.at[7], wx.at[11], at_z(z + 2), weight_sems[3])
            else:
                wt[6] = wt[4] + (wx[6] + wx[7] + wx[8] + wx[9]) + (wx[10] + wx[11])

        put_together(0)
        load_ours.start()
        pl.semaphore_wait(barrier, len(peers))
        swap_weight = swap(wt.at[0], wt.at[1], 16)
        swap_weight.start()
        gifts[0].start()
        for n in range(1, AHEAD):
            put_together(n)
            gifts[n].start()
        weights(0)
        load_ours.wait()

        def hand_over(low, i):
            part = fin.at[me, pl.ds(low, 2)]
            copy = swap(part, part, i)
            copy.start()
            return copy

        if me == 0:
            a, b, d, f = Mixed(0), Mixed(1), Flat(2), Flat(3)
            settle(0)
            a.one.far()
            settle(1)
            b.one.far()
            settle(2)
            settle(3)
            a.one.near()
            settle(4)
            settle(5)
            b.one.near()
            settle(6)
            settle(7)
            settle(8)
            settle(9)
            weights(1)
            a.one.relay()
            d.one.far()
            d.one.near()
            b.one.relay()
            f.one.far()
            settle(10)
            settle(11)
            f.one.near()
            settle(12)
            settle(13)
            settle(14)
            settle(15)
            a.end_one()
            a.step(0)
            a.step(1)
            b.end_one()
            b.step(0)
            b.step(1)
            d.one.relay()
            f.one.relay()
            a.step(2)
            a.step(3)
            b.step(2)
            b.step(3)
            a.step(4)
            a.step(5)
            b.step(4)
            b.step(5)
            weights(2)
            d.part(0)
            f.part(0)
            d.part(1)
            f.part(1)
            d.part(2)
            f.part(2)
            a.step(6)
            b.step(6)
            d.two.relay()
            f.two.relay()
            d.end_two()
            f.end_two()
            weights(3)
            a.end_two()
            b.end_two()
            d.relay_z()
            f.relay_z()
            a.end()
            b.end()
            first_swap = hand_over(0, 17)
            d.end()
            f.end()
            last_swap = hand_over(2, 18)
        else:
            a, b, c, e = Flat(0), Flat(1), Deep(2), Deep(3)
            settle(0)
            c.step(0, (1,))
            settle(1)
            c.step(0, (-1,))
            settle(2)
            e.step(0, (1,))
            settle(3)
            e.step(0, (-1,))
            settle(4)
            settle(5)
            c.step(1)
            c.step(2)
            settle(6)
            settle(7)
            e.step(1)
            e.step(2)
            weights(1)
            settle(8)
            settle(9)
            c.step(3)
            settle(10)
            settle(11)
            settle(12)
            c.step(4)
            settle(13)
            settle(14)
            e.step(3)
            settle(15)
            e.step(4)
            weights(2)
            a.one.far()
            b.one.far()
            a.one.near()
            b.one.near()
            c.step(5)
            e.step(5)
            c.step(6)
            e.step(6)
            a.one.relay()
            b.one.relay()
            a.part(0)
            b.part(0)
            a.part(1)
            b.part(1)
            a.part(2)
            b.part(2)
            a.two.relay()
            b.two.relay()
            c.end_one()
            c.two.far()
            c.two.near()
            e.end_one()
            e.two.far()
            e.two.near()
            a.end_two()
            b.end_two()
            weights(3)
            c.two.relay()
            e.two.relay()
            a.relay_z()
            b.relay_z()
            c.end_two()
            e.end_two()
            a.end()
            b.end()
            first_swap = hand_over(0, 17)
            c.end()
            e.end()
            last_swap = hand_over(2, 18)
        copy_to(partner, give, give, swap_send.at[0], swap_recv.at[0]).wait_send()
        swap_weight.wait_send()
        for group in groups:
            group.drain()
        assert len(groups) <= N_SEND and len(recvs) <= N_RECV
        for i in (17, 18):
            theirs_fin = fin.at[1 - me, pl.ds(2 * (i - 17), 2)]
            swap(theirs_fin, theirs_fin, i).wait_recv()
        weights(4)
        total = wt[6]
        for odd in (0, 1):
            @pl.when(lax.rem(zl, 2) == odd)
            def _():
                low = 4 * odd + 14 * me
                for p in (0, 1):
                    for unit in range(4):
                        out[:, p, unit * 128:(unit + 1) * 128] = fin[p, unit, low:low + 14] / total[:1]
        first_swap.wait_send()
        last_swap.wait_send()

    for me in (0, 1):
        @pl.when(core == me)
        def _():
            program(me)


def merge(deltas, ages, table):
    vmem = lambda *shape: pltpu.VMEM(shape, F32)
    return pl.pallas_call(
        kernel,
        out_shape=pltpu.VMEM((14, 2, 512), F32),
        in_specs=[
            pl.BlockSpec(memory_space=pltpu.HBM),
            pl.BlockSpec(memory_space=pltpu.HBM),
            pl.BlockSpec(memory_space=pltpu.HBM),
        ],
        out_specs=pl.BlockSpec(memory_space=pltpu.VMEM),
        scratch_shapes=[
            pltpu.SMEM((1,), jnp.int32),
            pltpu.SMEM((8,), F32),
            pltpu.VMEM((3584, 512), jnp.bfloat16),
            pltpu.VMEM((3584, 512), jnp.bfloat16),
            vmem(4, 32, BLOCK, 128),
            vmem(4, 32, BLOCK, 128),
            vmem(4, 32, BLOCK, 128),
            vmem(4, 3, 2, 4, BLOCK, 128),
            vmem(4, 3, 2, BLOCK, 128),
            vmem(2, 2, 7, 8, WIN, 128),
            vmem(2, 2, 7, 2, WIN, 128),
            vmem(2, 3, 2, 2, WIN, 128),
            vmem(4, 7, WIN, 128),
            vmem(4, 2, 4, BLOCK, 128),
            vmem(2, 16, WIN, 128),
            vmem(4, 2, BLOCK, 128),
            vmem(2, 7, WIN, 128),
            vmem(2, 7, WIN, 128),
            vmem(2, 4, WIN, 128),
            vmem(7, 8, 128),
            vmem(12, 8, 128),
            pltpu.SemaphoreType.DMA((N_SEND,)),
            pltpu.SemaphoreType.DMA((N_RECV,)),
            pltpu.SemaphoreType.DMA((4,)),
            pltpu.SemaphoreType.DMA((19,)),
            pltpu.SemaphoreType.DMA((7,)),
        ],
        compiler_params=pltpu.CompilerParams(
            collective_id=0, has_side_effects=True, vmem_limit_bytes=60 * 2**20),
        name="merge",
    )(deltas, ages.reshape(1), table)


def local(deltas, ages, table, params, momentum):
    merged = jnp.transpose(merge(deltas, ages, table), (1, 0, 2))
    new_momentum = momentum_decay * momentum + merged
    new_params = params - outer_rate * (merged + momentum_decay * new_momentum)
    return (new_params, new_momentum)


def solution(mesh):
    torus = Mesh(mesh.devices.reshape(2, 4, 4, 4, 2), ROW_COL)
    in_specs = (
        P(ROW_COL, None, None, None),
        P(ROW, COL),
        P(),
        P(None, ROW_COL, None),
        P(None, ROW_COL, None),
    )
    out_specs = (P(None, ROW_COL, None), P(None, ROW_COL, None))
    return jax.shard_map(local, mesh=torus, in_specs=in_specs, out_specs=out_specs, check_vma=False)
```

```python
import jax
import jax.numpy as jnp
from jax import lax
from jax.experimental import pallas as pl
from jax.experimental.pallas import tpu as pltpu
from jax.sharding import Mesh
from jax.sharding import PartitionSpec as P

ROW = ("z_hi", "y", "x")
COL = ("z_lo", "core")
ROW_COL = ROW + COL
MESH = pl.DeviceIdType.MESH
F32 = jnp.float32

momentum_decay = 0.9
outer_rate = 0.7

BLOCK = 112
WIN = 32
N_SEND, N_RECV = 13, 44
X, Y, ZX, ZY = "X", "Y", "ZX", "ZY"
KINDS = ((X, Y, X, Y), (X, Y, ZX, ZY))

ORDERS = (
    ((0, 2), (1, 2), (0, 1), (0, -1), (1, 1), (1, -1), (2, 2), (3, 2),
     (2, 1), (2, -1), (3, 1), (3, -1), (0, 0), (1, 0), (2, 0), (3, 0)),
    ((2, 1, 0), (2, 1, 1), (3, 1, 0), (3, 1, 1), (2, 0, 0), (2, 0, 1), (3, 0, 0), (3, 0, 1),
     (0, 2), (1, 2), (0, 1), (0, -1), (1, 1), (1, -1), (0, 0), (1, 0)),
)
AHEAD = 4
STRAIGHT = ((), (1,))


def wrap4(value):
    return lax.rem(value + 4, 4)


def kernel(delta, ages, table, out, age, levels, theirs, ours, give, got, mine, t1, t2, tc, tz, u2, zr,
           g1, g1c, g2, g2c, g2m, fin, wt, wx, send_sems, recv_sems, swap_send, swap_recv, load_sems):
    zh, y, x, zl, core = [lax.axis_index(name) for name in ROW_COL]
    z = zh * 4 + zl
    barrier = pltpu.get_barrier_semaphore()

    load_age = pltpu.make_async_copy(ages, age, load_sems.at[5])
    load_levels = pltpu.make_async_copy(table, levels, load_sems.at[6])
    load_age.start()
    load_levels.start()

    def program(me):
        kinds, other_kinds = KINDS[me], KINDS[1 - me]
        order, other_order = ORDERS[me], ORDERS[1 - me]

        def load(source, target, unit, sem):
            lanes = pl.ds(unit * 128, 128)
            return pltpu.make_async_copy(delta.at[0, source, :, lanes], target.at[:, lanes], load_sems.at[sem])

        first_use = list(dict.fromkeys(unit for unit, *_ in other_order))
        load_theirs = {unit: load(1 - me, theirs, unit, unit) for unit in first_use}
        load_ours = pltpu.make_async_copy(delta.at[0, me], ours, load_sems.at[4])
        for unit in first_use:
            load_theirs[unit].start()

        def at_z(there):
            there = lax.rem(there + 16, 8)
            return (there // 4, y, x, lax.rem(there, 4), me)

        def at_axis(axis, step):
            if axis == X:
                return (zh, y, wrap4(x + step), zl, me)
            return (zh, wrap4(y + step), x, zl, me)

        partner = (zh, y, x, zl, 1 - me)
        peers = [partner]
        peers += [at_axis(axis, s) for axis in (X, Y) for s in (1, 2, 3)]
        peers += [at_z(z + s) for s in (1, -1, 2, -2)]
        for peer in peers:
            pl.semaphore_signal(barrier, inc=1, device_id=peer, device_id_type=MESH)
        load_age.wait()
        load_levels.wait()
        weight = levels[age[0]]
        wt[0] = jnp.full((8, 128), weight, F32)

        def copy_to(device, src, dst, send_sem, recv_sem):
            return pltpu.make_async_remote_copy(
                src_ref=src, dst_ref=dst, send_sem=send_sem, recv_sem=recv_sem,
                device_id=device, device_id_type=MESH)

        groups, recvs = [], []

        def new_recv():
            recvs.append(len(recvs))
            return recv_sems.at[recvs[-1]]

        class Group:
            def __init__(self, whole):
                self.whole, self.send_sem = whole, send_sems.at[len(groups)]
                groups.append(self)

            def send(self, src, dst, device, recv_sem):
                copy = copy_to(device, src, dst, self.send_sem, recv_sem)
                copy.start()
                return copy

            def drain(self):
                copy_to(partner, self.whole, self.whole, self.send_sem, recv_sems.at[0]).wait_send()

        def arrived(whole, recv_sem):
            copy_to(partner, whole, whole, send_sems.at[0], recv_sem).wait_recv()

        def swap(src, dst, i):
            return copy_to(partner, src, dst, swap_send.at[max(i - 15, 0)], swap_recv.at[i])

        def position(axis):
            return x if axis == X else y

        def cross(axis):
            return Y if axis == X else X

        def term(src, unit, kind, slot):
            if kind in (ZX, ZY):
                half, d, j = slot // 16, lax.rem(slot, 16) // 4, lax.rem(slot, 4)
            else:
                d, half, j = slot // 8, lax.rem(slot, 8) // 4, lax.rem(slot, 4)
            block = half * 16 + (j * 4 + d if kind in (X, ZX) else d * 4 + j)
            start = pl.multiple_of(block * BLOCK, 16)
            return src[pl.ds(start, BLOCK), unit * 128:(unit + 1) * 128].astype(F32) * weight

        def chunk(kind, step):
            if kind in (ZX, ZY):
                return lax.rem(zh + step[0], 2) * 16 + 8 * step[1]
            return wrap4(position(kind) + step[0]) * 8

        gifts = []

        def put_together(n):
            unit, *step = other_order[n]
            kind = other_kinds[unit]
            if unit in load_theirs:
                load_theirs.pop(unit).wait()
            base = chunk(kind, step)

            @pl.loop(0, 8)
            def _(k):
                give[unit, base + k] = term(theirs, unit, kind, base + k)

            gifts.append(swap(give.at[unit, pl.ds(base, 8)], got.at[unit, pl.ds(base, 8)], n))

        def settle(n):
            if n + AHEAD < 16:
                put_together(n + AHEAD)
                gifts[-1].start()
            unit, *step = order[n]
            kind = kinds[unit]
            base = chunk(kind, step)
            swap(got.at[unit, pl.ds(base, 8)], got.at[unit, pl.ds(base, 8)], n).wait_recv()

            @pl.loop(0, 8)
            def _(k):
                mine[unit, base + k] = got[unit, base + k] + term(ours, unit, kind, base + k)

        class Tree:
            def __init__(self, piece, slots, axis):
                self.piece, self.slots, self.axis, self.at = piece, slots, axis, position(axis)
                self.group = Group(slots)
                self.first, self.rest = new_recv(), new_recv()

            def far(self):
                for s in (1, -1):
                    src = self.piece(int(s < 0), wrap4(self.at + 2))
                    dst = self.slots.at[0, int(s < 0)]
                    self.group.send(src, dst, at_axis(self.axis, s), self.first)

            def near(self):
                for s in (1, -1):
                    src = self.piece(int(s > 0), wrap4(self.at + s))
                    self.group.send(src, self.slots.at[1, int(s < 0)], at_axis(self.axis, s), self.rest)

            def relay(self):
                arrived(self.slots.at[0], self.first)
                for s in (1, -1):
                    held = self.slots.at[0, int(s < 0)]
                    held[...] = held[...] + self.piece(int(s < 0), wrap4(self.at + s))[...]
                    self.group.send(held, self.slots.at[2, int(s < 0)], at_axis(self.axis, s), self.rest)

            def finish(self, put):
                arrived(self.slots.at[pl.ds(1, 2)], self.rest)
                for h in (0, 1):
                    put(h, self.piece(h, self.at)[...] + self.slots[2, h] + self.slots[1, 1 - h])

        def window(there):
            there = lax.rem(there + 16, 8)
            low = lax.rem(there, 4)
            return there // 4, pl.multiple_of((low // 2) * 56 + lax.rem(low, 2) * 24, 8)

        class Quarters(Tree):
            def __init__(self, piece, slots, axis):
                super().__init__(piece, slots, axis)
                self.beside = position(cross(axis))
                self.parts = {step: new_recv() for step in (2, 1, -1, 0)}

            def relay(self):
                arrived(self.slots.at[0], self.first)
                for s in (1, -1):
                    k = int(s < 0)
                    held = self.slots.at[0, k]
                    held[...] = held[...] + self.piece(k, wrap4(self.at + s))[...]
                    for step, sem in self.parts.items():
                        j = wrap4(self.beside + step)
                        self.group.send(held.at[j], self.slots.at[2, k, j], at_axis(self.axis, s), sem)

            def part(self, step, put):
                if step == 2:
                    arrived(self.slots.at[1], self.rest)
                j = wrap4(self.beside + step)
                arrived(self.slots.at[2, :, j], self.parts[step])
                for h in (0, 1):
                    put(h, j, self.piece(h, self.at)[j] + self.slots[2, h, j] + self.slots[1, 1 - h, j])

        class Flat:
            def __init__(self, unit):
                axis = kinds[unit]
                self.unit = unit
                self.one = Quarters(lambda h, d: mine.at[unit, pl.ds(d * 8 + h * 4, 4)], t1.at[unit], axis)
                self.two = Tree(lambda h, d: g1.at[unit, h, d], t2.at[unit], cross(axis))
                self.group, self.last, self.far_sem = Group(zr.at[unit]), new_recv(), new_recv()
                self.way = 1 if unit % 2 == 0 else -1

            def part(self, n):
                def put(h, j, value):
                    g1[self.unit, h, j] = value
                for step in ((2,), (1, -1), (0,))[n]:
                    self.one.part(step, put)
                if n == 0:
                    self.two.far()
                elif n == 1:
                    self.two.near()

            def end_two(self):
                def put(h, value):
                    g2[self.unit, h] = value
                self.two.finish(put)
                if self.unit in STRAIGHT[me]:
                    for s in (4, 3, -3, 2, -2, 1, -1):
                        self.send_z(s, s, (s - 1) % 8, self.last)
                    return
                self.send_z(4, 2 * self.way, 4, self.far_sem)
                for s in (1, -1):
                    self.send_z(3 * s, s, 5 + int(s < 0), self.far_sem)
                for s in (1, -1):
                    self.send_z(s, s, int(s < 0), self.last)

            def piece_z(self, there):
                half, start = window(there)
                return g2.at[self.unit, half, pl.ds(start, WIN)]

            def send_z(self, there, step, slot, sem):
                self.group.send(self.piece_z(z + there), zr.at[self.unit, slot], at_z(z + step), sem)

            def relay_z(self):
                if self.unit in STRAIGHT[me]:
                    return
                arrived(zr.at[self.unit, pl.ds(4, 3)], self.far_sem)
                for s in (1, -1):
                    held = zr.at[self.unit, 5 + int(s < 0)]
                    value = held[...] + self.piece_z(z + 2 * s)[...]
                    if s == self.way:
                        value = value + zr[self.unit, 4]
                    held[...] = value
                    self.group.send(held, zr.at[self.unit, 2 + int(s < 0)], at_z(z + 2 * s), self.last)

            def end(self):
                count = 7 if self.unit in STRAIGHT[me] else 4
                arrived(zr.at[self.unit, pl.ds(0, count)], self.last)
                value = self.piece_z(z)[...]
                for n in range(count):
                    value = value + zr[self.unit, n]
                fin[me, self.unit] = value

        class Ring:
            dist = (4, 3, 3, 2, 2, 1, 1)

            def __init__(self, piece, slots):
                self.piece, self.slots = piece, slots
                self.group, self.sems = Group(slots), [new_recv() for _ in self.dist]

            def step(self, i, ways=(1, -1)):
                if i >= 2:
                    arrived(self.slots.at[:, i - 2], self.sems[i - 2])
                for s in ways:
                    k = int(s < 0)
                    piece = self.piece(z + s * self.dist[i], k if i % 2 == 0 else 1 - k)
                    if i >= 2:
                        held = self.slots.at[k, i - 2]
                        held[...] = held[...] + piece[...]
                        piece = held
                    self.group.send(piece, self.slots.at[k, i], at_z(z + s), self.sems[i])

            def finish(self, put):
                for i in (5, 6):
                    arrived(self.slots.at[:, i], self.sems[i])
                for half in (0, 1):
                    put(half, self.piece(z, half)[...] + self.slots[half, 6] + self.slots[1 - half, 5])

        class Direct:
            def __init__(self, held, axis, unit):
                self.held, self.axis, self.unit = held, axis, unit
                self.group, self.sem = Group(held.at[pl.ds(4, 3)]), new_recv()

            def start(self):
                for s in (2, 1, 3):
                    src = self.held.at[wrap4(position(self.axis) + s)]
                    self.group.send(src, self.held.at[3 + s], at_axis(self.axis, s), self.sem)

            def end(self):
                arrived(self.held.at[pl.ds(4, 3)], self.sem)
                own = self.held[position(self.axis)]
                fin[me, self.unit] = own + (self.held[4] + self.held[5] + self.held[6])

        class Deep:
            def __init__(self, unit):
                n = unit - 2
                axis = X if kinds[unit] == ZX else Y

                def piece(there, half):
                    up, start = window(there)
                    return mine.at[unit, pl.ds(up * 16 + half * 8, 8), pl.ds(start, WIN)]

                self.n, self.one = n, Ring(piece, tc.at[n])
                self.two = Tree(lambda h, d: g1c.at[n, pl.ds(d * 4 + h * 2, 2)], u2.at[n], axis)
                self.last = Direct(g2c.at[n], cross(axis), unit)
                self.step, self.end = self.one.step, self.last.end

            def end_one(self):
                def put(half, value):
                    g1c[self.n, half * 8:half * 8 + 8] = value
                self.one.finish(put)

            def end_two(self):
                def put(h, value):
                    g2c[self.n, h * 2:h * 2 + 2] = value
                self.two.finish(put)
                self.last.start()

        class Mixed:
            def __init__(self, unit):
                axis = kinds[unit]

                def piece(there, half):
                    up, start = window(there)
                    return g1.at[unit, up, pl.ds(half * 2, 2), pl.ds(start, WIN)]

                self.unit = unit
                self.one = Tree(lambda h, d: mine.at[unit, pl.ds(d * 8 + h * 4, 4)], t1.at[unit], axis)
                self.two = Ring(piece, tz.at[unit])
                self.last = Direct(g2m.at[unit], cross(axis), unit)
                self.step, self.end = self.two.step, self.last.end

            def end_one(self):
                def put(h, value):
                    g1[self.unit, h] = value
                self.one.finish(put)

            def end_two(self):
                def put(half, value):
                    g2m[self.unit, half * 2:half * 2 + 2] = value
                self.two.finish(put)
                self.last.start()

        weight_group, weight_sems = Group(wx), [new_recv() for _ in range(4)]

        def spread(value, slots, devices, stage):
            wt[2 + stage] = value
            for slot, device in zip(slots, devices):
                weight_group.send(wt.at[2 + stage], wx.at[slot], device, weight_sems[stage])

        def weights(stage):
            if stage == 0:
                swap(wt.at[1], wt.at[1], 16).wait_recv()
                return spread(wt[0] + wt[1], (0, 1, 2), [at_axis(X, s) for s in (1, 2, 3)], 0)
            low, count = ((0, 3), (3, 3), (6, 4), (10, 2))[stage - 1]
            arrived(wx.at[pl.ds(low, count)], weight_sems[stage - 1])
            if stage == 1:
                spread(wt[2] + wx[0] + wx[1] + wx[2], (3, 4, 5), [at_axis(Y, s) for s in (1, 2, 3)], 1)
            elif stage == 2:
                spread(wt[3] + wx[3] + wx[4] + wx[5], (6, 7, 8, 9), [at_z(z + s) for s in (-1, 1, -2, 2)], 2)
            elif stage == 3:
                wt[5] = wx[6] + wx[8]
                weight_group.send(wt.at[5], wx.at[10], at_z(z - 2), weight_sems[3])
                weight_group.send(wx.at[7], wx.at[11], at_z(z + 2), weight_sems[3])
            else:
                wt[6] = wt[4] + (wx[6] + wx[7] + wx[8] + wx[9]) + (wx[10] + wx[11])

        put_together(0)
        load_ours.start()
        pl.semaphore_wait(barrier, len(peers))
        swap_weight = swap(wt.at[0], wt.at[1], 16)
        swap_weight.start()
        gifts[0].start()
        for n in range(1, AHEAD):
            put_together(n)
            gifts[n].start()
        weights(0)
        load_ours.wait()

        def hand_over(low, i):
            part = fin.at[me, pl.ds(low, 2)]
            copy = swap(part, part, i)
            copy.start()
            return copy

        if me == 0:
            a, b, d, f = Mixed(0), Mixed(1), Flat(2), Flat(3)
            settle(0)
            a.one.far()
            settle(1)
            b.one.far()
            settle(2)
            settle(3)
            a.one.near()
            settle(4)
            settle(5)
            b.one.near()
            settle(6)
            settle(7)
            settle(8)
            settle(9)
            weights(1)
            a.one.relay()
            d.one.far()
            d.one.near()
            b.one.relay()
            f.one.far()
            settle(10)
            settle(11)
            f.one.near()
            settle(12)
            settle(13)
            settle(14)
            settle(15)
            a.end_one()
            a.step(0)
            a.step(1)
            b.end_one()
            b.step(0)
            b.step(1)
            d.one.relay()
            f.one.relay()
            a.step(2)
            a.step(3)
            b.step(2)
            b.step(3)
            a.step(4)
            a.step(5)
            b.step(4)
            b.step(5)
            weights(2)
            d.part(0)
            f.part(0)
            d.part(1)
            f.part(1)
            d.part(2)
            f.part(2)
            a.step(6)
            b.step(6)
            d.two.relay()
            f.two.relay()
            d.end_two()
            f.end_two()
            weights(3)
            a.end_two()
            b.end_two()
            d.relay_z()
            f.relay_z()
            a.end()
            b.end()
            first_swap = hand_over(0, 17)
            d.end()
            f.end()
            last_swap = hand_over(2, 18)
        else:
            a, b, c, e = Flat(0), Flat(1), Deep(2), Deep(3)
            settle(0)
            c.step(0, (1,))
            settle(1)
            c.step(0, (-1,))
            settle(2)
            e.step(0, (1,))
            settle(3)
            e.step(0, (-1,))
            settle(4)
            settle(5)
            c.step(1)
            c.step(2)
            settle(6)
            settle(7)
            e.step(1)
            e.step(2)
            weights(1)
            settle(8)
            settle(9)
            c.step(3)
            settle(10)
            settle(11)
            settle(12)
            c.step(4)
            settle(13)
            settle(14)
            e.step(3)
            settle(15)
            e.step(4)
            weights(2)
            a.one.far()
            b.one.far()
            a.one.near()
            b.one.near()
            c.step(5)
            e.step(5)
            c.step(6)
            e.step(6)
            a.one.relay()
            b.one.relay()
            a.part(0)
            b.part(0)
            a.part(1)
            b.part(1)
            a.part(2)
            b.part(2)
            a.two.relay()
            b.two.relay()
            c.end_one()
            c.two.far()
            c.two.near()
            e.end_one()
            e.two.far()
            e.two.near()
            a.end_two()
            b.end_two()
            weights(3)
            c.two.relay()
            e.two.relay()
            a.relay_z()
            b.relay_z()
            c.end_two()
            e.end_two()
            a.end()
            b.end()
            first_swap = hand_over(0, 17)
            c.end()
            e.end()
            last_swap = hand_over(2, 18)
        copy_to(partner, give, give, swap_send.at[0], swap_recv.at[0]).wait_send()
        swap_weight.wait_send()
        for group in groups:
            group.drain()
        assert len(groups) <= N_SEND and len(recvs) <= N_RECV
        for i in (17, 18):
            theirs_fin = fin.at[1 - me, pl.ds(2 * (i - 17), 2)]
            swap(theirs_fin, theirs_fin, i).wait_recv()
        weights(4)
        total = wt[6]
        for odd in (0, 1):
            @pl.when(lax.rem(zl, 2) == odd)
            def _():
                low = 4 * odd + 14 * me
                for p in (0, 1):
                    for unit in range(4):
                        out[:, p, unit * 128:(unit + 1) * 128] = fin[p, unit, low:low + 14] / total[:1]
        first_swap.wait_send()
        last_swap.wait_send()

    for me in (0, 1):
        @pl.when(core == me)
        def _():
            program(me)


def merge(deltas, ages, table):
    vmem = lambda *shape: pltpu.VMEM(shape, F32)
    return pl.pallas_call(
        kernel,
        out_shape=pltpu.VMEM((14, 2, 512), F32),
        in_specs=[
            pl.BlockSpec(memory_space=pltpu.HBM),
            pl.BlockSpec(memory_space=pltpu.HBM),
            pl.BlockSpec(memory_space=pltpu.HBM),
        ],
        out_specs=pl.BlockSpec(memory_space=pltpu.VMEM),
        scratch_shapes=[
            pltpu.SMEM((1,), jnp.int32),
            pltpu.SMEM((8,), F32),
            pltpu.VMEM((3584, 512), jnp.bfloat16),
            pltpu.VMEM((3584, 512), jnp.bfloat16),
            vmem(4, 32, BLOCK, 128),
            vmem(4, 32, BLOCK, 128),
            vmem(4, 32, BLOCK, 128),
            vmem(4, 3, 2, 4, BLOCK, 128),
            vmem(4, 3, 2, BLOCK, 128),
            vmem(2, 2, 7, 8, WIN, 128),
            vmem(2, 2, 7, 2, WIN, 128),
            vmem(2, 3, 2, 2, WIN, 128),
            vmem(4, 7, WIN, 128),
            vmem(4, 2, 4, BLOCK, 128),
            vmem(2, 16, WIN, 128),
            vmem(4, 2, BLOCK, 128),
            vmem(2, 7, WIN, 128),
            vmem(2, 7, WIN, 128),
            vmem(2, 4, WIN, 128),
            vmem(7, 8, 128),
            vmem(12, 8, 128),
            pltpu.SemaphoreType.DMA((N_SEND,)),
            pltpu.SemaphoreType.DMA((N_RECV,)),
            pltpu.SemaphoreType.DMA((4,)),
            pltpu.SemaphoreType.DMA((19,)),
            pltpu.SemaphoreType.DMA((7,)),
        ],
        compiler_params=pltpu.CompilerParams(
            collective_id=0, has_side_effects=True, vmem_limit_bytes=60 * 2**20),
        name="merge",
    )(deltas, ages.reshape(1), table)


def local(deltas, ages, table, params, momentum):
    merged = jnp.transpose(merge(deltas, ages, table), (1, 0, 2))
    new_momentum = momentum_decay * momentum + merged
    new_params = params - outer_rate * (merged + momentum_decay * new_momentum)
    return (new_params, new_momentum)


def solution(mesh):
    torus = Mesh(mesh.devices.reshape(2, 4, 4, 4, 2), ROW_COL)
    in_specs = (
        P(ROW_COL, None, None, None),
        P(ROW, COL),
        P(),
        P(None, ROW_COL, None),
        P(None, ROW_COL, None),
    )
    out_specs = (P(None, ROW_COL, None), P(None, ROW_COL, None))
    return jax.shard_map(local, mesh=torus, in_specs=in_specs, out_specs=out_specs, check_vma=False)
```
